32 devices in a mesh: dp: 1 (over z), tp: 4 (over y), fsdp: 8 (over x, core).
Axes of the slice: x: 4, y: 4, z: 1, core: 2. Of those that a mesh axis runs over, the one named last changes fastest.
The devices are a block of a 4x4x8 slice.
Arguments:
- tokens: bfloat16 [8, 2048, 4096], P(('dp', 'fsdp'))
- positions: int32 [8, 2048], P(('dp', 'fsdp'))
- valid_len: int32 [8], P(('dp', 'fsdp'))
- w_query: bfloat16 [4096, 4096], P('fsdp', 'tp')
- w_key: bfloat16 [4096, 1024], P('fsdp', 'tp')
- w_value: bfloat16 [4096, 1024], P('fsdp', 'tp')
- w_out: bfloat16 [4096, 4096], P('tp', 'fsdp')
- w_gate: bfloat16 [4096, 14336], P('fsdp', 'tp')
- w_up: bfloat16 [4096, 14336], P('fsdp', 'tp')
- w_down: bfloat16 [14336, 4096], P('tp', 'fsdp')
- norm_attn: bfloat16 [4096], replicated
- norm_mlp: bfloat16 [4096], replicated
Outputs:
- output 1: bfloat16 [8, 2048, 4096], P(('dp', 'fsdp'))
- output 2: bfloat16 [8, 2048, 8, 128], P(('dp', 'fsdp'), None, 'tp')
- output 3: bfloat16 [8, 2048, 8, 128], P(('dp', 'fsdp'), None, 'tp')
All inputs are finite; a program needn't handle non-finite values.
Results may differ from the reference program's by a relative error of at most 0.0135249.
Values are sent between devices in bfloat16 or wider.
A program may use at most 768 MiB of HBM per device.

```python
import math
import jax
import jax.numpy as jnp
from jax import lax

MODEL_DIM = 4096
Q_HEADS = 32
KV_HEADS = 8
HEAD_DIM = 128
FFN_DIM = 14336
SEQ_LEN = 2048
BATCH_SIZE = 8

GROUP_SIZE = Q_HEADS // KV_HEADS
Q_BLOCK = min(SEQ_LEN, 256)
ROPE_THETA = 500000.0
NORM_EPS = 1e-5
SCORE_SCALE = HEAD_DIM ** -0.5
Q_GAIN = math.sqrt(max(math.log(SEQ_LEN) - 2.5, 1.0))


def setup_inputs(seed: int = 0, part: int = 0) -> dict:
    part_key = jax.random.fold_in(jax.random.key(seed), part)
    key_tok, key_pos, key_len = jax.random.split(part_key, 3)
    w_keys = jax.random.split(jax.random.key(seed + 1), 9)

    def draw_matrix(sub_key, mat_shape, scale_by):
        return (jax.random.normal(sub_key, mat_shape, jnp.float32) * scale_by).astype(jnp.bfloat16)

    tokens = jax.random.normal(key_tok, (BATCH_SIZE, SEQ_LEN, MODEL_DIM), jnp.float32).astype(jnp.bfloat16)
    starts = jax.random.randint(key_pos, (BATCH_SIZE, 1), 0, 4 * SEQ_LEN + 1, dtype=jnp.int32)
    positions = starts + jnp.arange(SEQ_LEN, dtype=jnp.int32)[None, :]
    valid_len = jax.random.randint(key_len, (BATCH_SIZE,), 1, SEQ_LEN + 1, dtype=jnp.int32).at[0].set(SEQ_LEN)
    q_width = Q_HEADS * HEAD_DIM
    kv_width = KV_HEADS * HEAD_DIM
    return {
        'tokens': tokens,
        'positions': positions,
        'valid_len': valid_len,
        'w_query': draw_matrix(w_keys[0], (MODEL_DIM, q_width), Q_GAIN * MODEL_DIM ** -0.5),
        'w_key': draw_matrix(w_keys[1], (MODEL_DIM, kv_width), MODEL_DIM ** -0.5),
        'w_value': draw_matrix(w_keys[2], (MODEL_DIM, kv_width), MODEL_DIM ** -0.5),
        'w_out': draw_matrix(w_keys[3], (q_width, MODEL_DIM), q_width ** -0.5),
        'w_gate': draw_matrix(w_keys[4], (MODEL_DIM, FFN_DIM), MODEL_DIM ** -0.5),
        'w_up': draw_matrix(w_keys[5], (MODEL_DIM, FFN_DIM), MODEL_DIM ** -0.5),
        'w_down': draw_matrix(w_keys[6], (FFN_DIM, MODEL_DIM), FFN_DIM ** -0.5),
        'norm_attn': (1.0 + 0.4 * jax.random.normal(w_keys[7], (MODEL_DIM,), jnp.float32)).astype(jnp.bfloat16),
        'norm_mlp': (1.0 + 0.4 * jax.random.normal(w_keys[8], (MODEL_DIM,), jnp.float32)).astype(jnp.bfloat16),
    }


def rope_freqs():
    half_idx = jnp.arange(HEAD_DIM // 2, dtype=jnp.float32)
    inv_freq = jnp.power(ROPE_THETA, -2.0 * half_idx / HEAD_DIM)
    wave_len = 2.0 * math.pi / inv_freq
    smooth = (8192.0 / wave_len - 1.0) / 3.0
    blended = (1.0 - smooth) * inv_freq / 8.0 + smooth * inv_freq
    return jnp.where(wave_len < 2048.0, inv_freq, jnp.where(wave_len > 8192.0, inv_freq / 8.0, blended))


def rms_norm(values, gain_vec):
    vals_f32 = values.astype(jnp.float32)
    inv_rms = lax.rsqrt(jnp.mean(vals_f32 * vals_f32, axis=-1, keepdims=True) + NORM_EPS)
    return (vals_f32 * inv_rms * gain_vec.astype(jnp.float32)).astype(jnp.bfloat16)


def rotate(proj_val, cos_t, sin_t):
    half_dim = proj_val.shape[-1] // 2
    lead_half = proj_val[..., :half_dim]
    tail_half = proj_val[..., half_dim:]
    return jnp.concatenate([lead_half * cos_t - tail_half * sin_t, tail_half * cos_t + lead_half * sin_t], axis=-1)


def reference(tokens, positions, valid_len, w_query, w_key, w_value, w_out, w_gate, w_up, w_down, norm_attn, norm_mlp):
    inv_freqs = rope_freqs()
    key_idx = jnp.arange(SEQ_LEN)
    n_blocks = SEQ_LEN // Q_BLOCK

    def one_request(request_data):
        x_req, pos_req, req_len = request_data
        angles = pos_req.astype(jnp.float32)[:, None] * inv_freqs[None, :]
        cos_t = jnp.cos(angles)[:, None, :]
        sin_t = jnp.sin(angles)[:, None, :]
        h_in = rms_norm(x_req, norm_attn)
        q_proj = jnp.dot(h_in, w_query, preferred_element_type=jnp.float32).reshape(SEQ_LEN, Q_HEADS, HEAD_DIM)
        k_proj = jnp.dot(h_in, w_key, preferred_element_type=jnp.float32).reshape(SEQ_LEN, KV_HEADS, HEAD_DIM)
        v_req = jnp.dot(h_in, w_value, preferred_element_type=jnp.float32).astype(jnp.bfloat16).reshape(SEQ_LEN, KV_HEADS, HEAD_DIM)
        q_rot = rotate(q_proj, cos_t, sin_t).astype(jnp.bfloat16)
        k_rot = rotate(k_proj, cos_t, sin_t).astype(jnp.bfloat16)
        q_blocks = q_rot.reshape(n_blocks, Q_BLOCK, KV_HEADS, GROUP_SIZE, HEAD_DIM)
        k_f32 = k_rot.astype(jnp.float32)
        v_f32 = v_req.astype(jnp.float32)

        def one_block(block_data):
            q_blk, first_row = block_data
            scores = jnp.einsum('qkgd,skd->kgqs', q_blk.astype(jnp.float32), k_f32) * SCORE_SCALE
            q_idx = first_row + jnp.arange(Q_BLOCK)
            allowed = (key_idx[None, :] <= q_idx[:, None]) & (key_idx[None, :] < req_len)
            scores = jnp.where(allowed, scores, -jnp.inf)
            attn_prob = jax.nn.softmax(scores, axis=-1).astype(jnp.bfloat16).astype(jnp.float32)
            return jnp.einsum('kgqs,skd->qkgd', attn_prob, v_f32).astype(jnp.bfloat16)

        blocks = lax.map(one_block, (q_blocks, jnp.arange(n_blocks) * Q_BLOCK))
        attn_out = blocks.reshape(SEQ_LEN, Q_HEADS * HEAD_DIM)
        y_attn = jnp.dot(attn_out, w_out, preferred_element_type=jnp.float32)
        resid_mid = (x_req.astype(jnp.float32) + y_attn).astype(jnp.bfloat16)
        h_mlp = rms_norm(resid_mid, norm_mlp)
        gate_val = jnp.dot(h_mlp, w_gate, preferred_element_type=jnp.float32)
        up_val = jnp.dot(h_mlp, w_up, preferred_element_type=jnp.float32)
        hidden_act = (jax.nn.silu(gate_val) * up_val).astype(jnp.bfloat16)
        down_val = jnp.dot(hidden_act, w_down, preferred_element_type=jnp.float32)
        out_req = (resid_mid.astype(jnp.float32) + down_val).astype(jnp.bfloat16)
        return out_req, k_rot, v_req

    hidden_out, key_cache, value_cache = lax.map(one_request, (tokens, positions, valid_len))
    return hidden_out, key_cache, value_cache
```

```python
import functools
import math
import jax
import jax.numpy as jnp
from jax import lax
from jax.experimental import pallas as pl
from jax.experimental.pallas import tpu as pltpu
from jax.sharding import PartitionSpec as P

HEAD_DIM = 128
ROPE_THETA = 500000.0
NORM_EPS = 1e-5
SCORE_SCALE = HEAD_DIM ** -0.5
LOG2E = 1.4426950408889634
BF16 = jnp.bfloat16
F32 = jnp.float32
N_REL = 4
N_ROWCH = 4
N_DOWN = 4
TILE = 256
GU_SPLIT = (0, 2, 6, 10, 14)
MESH = pl.DeviceIdType.MESH
VMEM_PLACE = 50331648


def rope_freqs():
    half_idx = jnp.arange(HEAD_DIM // 2, dtype=F32)
    inv_freq = jnp.power(ROPE_THETA, -2.0 * half_idx / HEAD_DIM)
    wave_len = 2.0 * math.pi / inv_freq
    smooth = (8192.0 / wave_len - 1.0) / 3.0
    blended = (1.0 - smooth) * inv_freq / 8.0 + smooth * inv_freq
    return jnp.where(wave_len < 2048.0, inv_freq, jnp.where(wave_len > 8192.0, inv_freq / 8.0, blended))


def layer_kernel(n_tp, n_fsdp, *refs):
    (pos_ref, len_ref, freq_ref, gains, tok, wk, wv, wq, wo, wg, wu, wd,
     kv_out, res, full_p, full_o, full_g, full_u, full_d, act, rs,
     u_buf, w_buf, p_buf, x1_buf, qkv_buf, o_buf, stage, r_buf, a_stage, cos_ref, sin_ref, bias_ref,
     x_send, x_recv, y_send, y_recv, w_sem, wd_sem, l_sem, b_sem, a_sem, r_sem, o_sem) = refs
    n_tok, width = tok.shape
    rows = n_tok // N_ROWCH
    sub = rows // N_REL
    k_rows = wk.shape[0]
    kv_cols = wk.shape[1]
    q_cols = wq.shape[1]
    ffn = wg.shape[1]
    o_cols = wo.shape[1]
    d_cols = wd.shape[1] // N_DOWN
    c_cols = d_cols * n_fsdp
    n_x = n_fsdp // 2

    me_t = lax.axis_index("tp")
    me_f = lax.axis_index("fsdp")
    chip, core = me_f // 2, me_f % 2
    t_right = lax.rem(me_t + 1, n_tp)
    t_left = lax.rem(me_t + n_tp - 1, n_tp)
    f_right = 2 * lax.rem(chip + 1, n_x) + core
    f_left = 2 * lax.rem(chip + n_x - 1, n_x) + core
    f_far = 2 * lax.rem(chip + 2, n_x) + core
    other = 1 - 2 * core
    f_twin = me_f + other

    barrier = pltpu.get_barrier_semaphore()
    for peer in ({"tp": t_left}, {"tp": t_right}, {"fsdp": f_left}, {"fsdp": f_right}, {"fsdp": f_twin}):
        pl.semaphore_signal(barrier, inc=1, device_id=peer, device_id_type=MESH)
    pl.semaphore_wait(barrier, 5)

    def al(val, mult):
        return pl.multiple_of(val, mult)

    pieces = []

    def add_piece(own, place):
        pieces.append((own, place, len(pieces) % 2))
        return len(pieces) - 1

    def by_rows(full, c0, c1):
        return lambda f: full.at[pl.ds(al(f * k_rows, k_rows), k_rows), pl.ds(c0, c1 - c0)]

    def halves(own, place):
        n = own.shape[0] // 2
        return tuple(add_piece(own.at[pl.ds(i * n, n), :], lambda f, i=i: place(f).at[pl.ds(i * n, n), :]) for i in range(2))

    def cols_of(own, full, c0, c1):
        return add_piece(own.at[:, pl.ds(c0, c1 - c0)], by_rows(full, c0, c1))

    half_q = q_cols // 2
    q_from = 2 * kv_cols
    pk = add_piece(wk, by_rows(full_p, 0, kv_cols))
    pv = add_piece(wv, by_rows(full_p, kv_cols, q_from))
    q0, q1 = [add_piece(wq.at[:, pl.ds(c, half_q)], by_rows(full_p, q_from + c, q_from + c + half_q)) for c in (0, half_q)]
    po = halves(wo, lambda f: full_o.at[:, pl.ds(al(f * o_cols, o_cols), o_cols)])
    pg = [tuple(cols_of(own, full, lo * TILE, hi * TILE) for own, full in ((wg, full_g), (wu, full_u)))
          for lo, hi in zip(GU_SPLIT, GU_SPLIT[1:])]
    pd = [halves(wd.at[:, pl.ds(k * d_cols, d_cols)], lambda f, k=k: full_d.at[k, :, pl.ds(al(f * d_cols, d_cols), d_cols)])
          for k in range(N_DOWN)]

    def x_copy(p, m):
        own, place, way = pieces[p]
        if m in (0, 1, 3):
            src, owner = own, me_f
        elif m == 2:
            owner = f_left if way == 0 else f_right
            src = place(owner)
        else:
            owner = {4: f_left, 5: f_right, 6: f_far}[m]
            src = place(owner)
        target = {0: f_right, 1: f_left, 2: f_right if way == 0 else f_left}.get(m, f_twin)
        return pltpu.make_async_remote_copy(src_ref=src, dst_ref=place(owner), send_sem=x_send.at[p, m], recv_sem=x_recv.at[p, m],
                                            device_id={"fsdp": target}, device_id_type=MESH)

    def x_wait(p, m):
        own, place, _ = pieces[p]
        owner = {0: f_left, 1: f_right, 2: f_far, 3: me_f + other, 4: f_left + other, 5: f_right + other, 6: f_far + other}[m]
        pltpu.make_async_remote_copy(src_ref=own, dst_ref=place(owner), send_sem=x_send.at[p, m], recv_sem=x_recv.at[p, m],
                                     device_id={"fsdp": f_twin}, device_id_type=MESH).wait_recv()

    def x_first(*ps):
        for p in ps:
            for m in (0, 1, 3):
                x_copy(p, m).start()

    def x_fwd(*ps):
        for p in ps:
            way = pieces[p][2]
            x_wait(p, way)
            x_copy(p, 2).start()
            x_copy(p, 4 + way).start()

    def x_side(*ps):
        for p in ps:
            way = 1 - pieces[p][2]
            x_wait(p, way)
            x_copy(p, 4 + way).start()

    def x_second(*ps):
        x_fwd(*ps)
        x_side(*ps)

    def x_third(*ps):
        for p in ps:
            x_wait(p, 2)
            x_copy(p, 6).start()

    def x_ready(*ps):
        for p in ps:
            for m in (3, 4, 5, 6):
                x_wait(p, m)

    unit_list = [(k, pair) for pair in range(2) for k in range(N_DOWN)]
    unit_at = [2 * k + pair for k, pair in unit_list]
    unit_order = {u: i for i, u in enumerate(unit_at)}

    def y_rows(e):
        if e < N_ROWCH:
            slot, lane, wid = e % 2, 0, width
        else:
            q = unit_order[e - N_ROWCH] % 4
            slot, lane, wid = q // 2, (q % 2) * (width // 2), 2 * c_cols
        return slot, lane, wid

    def lanes(e, h):
        slot, lane, wid = y_rows(e)
        return slot, pl.ds(lane + h * (wid // 2), wid // 2), pl.ds(h * (wid // 2), wid // 2)

    def g_slice(e, r):
        if e < N_ROWCH:
            return u_buf.at[pl.ds(e * rows + r * sub, sub), :]
        return res.at[e - N_ROWCH, r]

    FAR, NEAR, SUM, RIGHT, LEFT, PASS = range(6)

    def y_copy(e, m, h=0):
        slot, here, there = lanes(e, h)
        if m in (RIGHT, LEFT):
            src, dst, to = g_slice(e, 0), g_slice(e, m - 2), m - 3
            if e >= N_ROWCH:
                src, dst = r_buf.at[unit_order[e - N_ROWCH] % 2, :, there], dst.at[:, there]
        elif m == PASS:
            src, dst, to = g_slice(e, 2 - h).at[:, there], g_slice(e, 3).at[:, there], 1 - h
        else:
            r, i, to = {FAR: (3, 0, h), NEAR: (1 + h, 2 - h, 1 - h), SUM: (2 - h, 1 + h, h)}[m]
            src, dst = p_buf.at[slot, pl.ds(r * sub, sub), here], rs.at[e, i, :, there]
        return pltpu.make_async_remote_copy(src_ref=src, dst_ref=dst, send_sem=y_send.at[e, m, h], recv_sem=y_recv.at[e, m, h],
                                            device_id={"tp": t_right if to == 0 else t_left}, device_id_type=MESH)

    def rs_slice(e, i):
        return rs.at[e, i, :, pl.ds(0, y_rows(e)[2])]

    def load_stage(e, idx):
        wid = y_rows(e)[2]
        for i in idx:
            pltpu.make_async_copy(rs_slice(e, i), stage.at[i, :, pl.ds(0, wid)], l_sem.at[i]).start()

    def wait_stage(e, idx):
        wid = y_rows(e)[2]
        for i in idx:
            pltpu.make_async_copy(rs_slice(e, i), stage.at[i, :, pl.ds(0, wid)], l_sem.at[i]).wait()

    def y_start(e, hs=(0, 1)):
        for m in (FAR, NEAR):
            for h in hs:
                y_copy(e, m, h).start()

    def y_have(e, hs=(0, 1)):
        for h in hs:
            y_copy(e, NEAR, h).wait_recv()
            y_copy(e, SUM, h).wait_recv()

    def y_send_all(e, hs=(0,)):
        for h in hs:
            y_copy(e, LEFT, h).start()
            y_copy(e, RIGHT, h).start()

    def y_sent_all(e, hs=(0,)):
        for h in hs:
            y_copy(e, LEFT, h).wait_send()
            y_copy(e, RIGHT, h).wait_send()

    EW = 32

    def y_add(e):
        for h in (0, 1):
            slot, here, there = lanes(e, h)
            y_copy(e, FAR, h).wait_recv()
            pltpu.make_async_copy(rs.at[e, 0, :, there], stage.at[0, :, there], l_sem.at[h]).start()
        for h in (0, 1):
            slot, here, there = lanes(e, h)
            pltpu.make_async_copy(rs.at[e, 0, :, there], stage.at[0, :, there], l_sem.at[h]).wait()

            def body(i, carry, h=h, here=here, there=there):
                rr = pl.ds(al((2 - h) * sub + i * EW, EW), EW)
                tot = p_buf[slot, rr, here].astype(F32) + stage[0, pl.ds(al(i * EW, EW), EW), there].astype(F32)
                p_buf[slot, rr, here] = tot.astype(BF16)
                return carry

            lax.fori_loop(0, sub // EW, body, 0)
            y_copy(e, SUM, h).start()

    def tok_copy(c):
        row0 = al(c * rows + me_t * sub, sub)
        return pltpu.make_async_copy(tok.at[pl.ds(row0, sub), :], stage.at[0], l_sem.at[3])

    def y_norm(c):
        slot = c % 2
        tok_copy(c).start()
        y_have(c)
        load_stage(c, (1, 2))
        wait_stage(c, (1, 2))
        tok_copy(c).wait()

        def body(i, carry):
            rr = al(i * EW, EW)
            here = pl.ds(rr, EW)
            tot = p_buf[slot, here, :].astype(F32) + stage[1, here, :].astype(F32) + stage[2, here, :].astype(F32)
            x1 = (stage[0, here, :].astype(F32) + tot).astype(BF16)
            x1_buf[pl.ds(al(c * sub + i * EW, EW), EW), :] = x1
            xf = x1.astype(F32)
            inv = lax.rsqrt(jnp.mean(xf * xf, axis=-1, keepdims=True) + NORM_EPS)
            u_buf[pl.ds(al(c * rows + i * EW, EW), EW), :] = (xf * inv * gains[1:, :]).astype(BF16)
            return carry

        lax.fori_loop(0, sub // EW, body, 0)
        y_send_all(c)

    def y_final(k, pair):
        unit = 2 * k + pair
        e = N_ROWCH + unit
        r_slot = unit_order[unit] % 2
        if unit_order[unit] >= 2:
            before = N_ROWCH + unit_at[unit_order[unit] - 2]
            y_sent_all(before, (0, 1))
            r_out(before).wait()
        for h in (0, 1):
            slot, mine, there = lanes(e, h)
            y_have(e, (h,))
            loads = [pltpu.make_async_copy(rs.at[e, i, :, there], stage.at[i, :, there], l_sem.at[i]) for i in (1, 2)]
            for cp in loads:
                cp.start()
            for cp in loads:
                cp.wait()

            def body(i, carry, h=h, slot=slot, mine=mine):
                here = pl.ds(al(i * EW, EW), EW)
                x_rows = pl.ds(al((2 * pair + h) * sub + i * EW, EW), EW)
                for f in range(n_fsdp):
                    at = pl.ds(h * c_cols + f * d_cols, d_cols)
                    tot = (p_buf[slot, here, pl.ds(mine.start + f * d_cols, d_cols)].astype(F32)
                           + stage[1, here, at].astype(F32) + stage[2, here, at].astype(F32))
                    x1 = x1_buf[x_rows, pl.ds((f * N_DOWN + k) * d_cols, d_cols)].astype(F32)
                    r_buf[r_slot, here, at] = (x1 + tot).astype(BF16)
                return carry

            lax.fori_loop(0, sub // EW, body, 0)
            y_send_all(e, (h,))
        r_out(e).start()

    def r_out(e):
        return pltpu.make_async_copy(r_buf.at[unit_order[e - N_ROWCH] % 2], res.at[e - N_ROWCH, 0], r_sem.at[unit_order[e - N_ROWCH] % 2])

    def y_pass(e):
        for h in (0, 1):
            y_copy(e, LEFT - h, h if e >= N_ROWCH else 0).wait_recv()
            y_copy(e, PASS, h).start()

    def y_ready(e):
        for h in (0, 1):
            if e >= N_ROWCH:
                y_copy(e, RIGHT + h, h).wait_recv()
            y_copy(e, PASS, h).wait_recv()

    def bounce(src, via, dst, i):
        return pltpu.make_async_copy(src, via, b_sem.at[0, i]), pltpu.make_async_copy(via, dst, b_sem.at[1, i])

    small = [
        bounce(wk, w_buf.at[0, pl.ds(0, k_rows), pl.ds(0, kv_cols)], pieces[pk][1](me_f), 0),
        bounce(wv, w_buf.at[0, pl.ds(0, k_rows), pl.ds(kv_cols, kv_cols)], pieces[pv][1](me_f), 1),
        bounce(wq.at[:, pl.ds(0, half_q)], w_buf.at[0, pl.ds(k_rows, k_rows), :], pieces[q0][1](me_f), 2),
        bounce(wq.at[:, pl.ds(half_q, half_q)], w_buf.at[0, pl.ds(2 * k_rows, k_rows), :], pieces[q1][1](me_f), 3),
        bounce(wo, w_buf.at[0, pl.ds(3 * k_rows, wo.shape[0]), :], full_o.at[:, pl.ds(al(me_f * o_cols, o_cols), o_cols)], 4),
    ] + [
        bounce(wd.at[:, pl.ds(k * d_cols, d_cols)], w_buf.at[1, pl.ds(0, ffn), pl.ds(k * d_cols, d_cols)], full_d.at[k, :, pl.ds(al(me_f * d_cols, d_cols), d_cols)], 5 + k)
        for k in range(N_DOWN)
    ]
    large = [
        bounce(wg, p_buf.at[0, :, pl.ds(0, ffn)], full_g.at[pl.ds(al(me_f * k_rows, k_rows), k_rows), :], 9),
        bounce(wu, p_buf.at[1, :, pl.ds(0, ffn)], full_u.at[pl.ds(al(me_f * k_rows, k_rows), k_rows), :], 10),
    ]

    def bounce_in(group):
        for a, _ in group:
            a.start()

    def bounce_out(group):
        for a, b in group:
            a.wait()
            b.start()

    def bounce_end(group):
        for _, b in group:
            b.wait()

    def norm_rows(late):
        n_tile = n_tok // rows

        def load(i):
            return pltpu.make_async_copy(tok.at[pl.ds(i * rows, rows), :], p_buf.at[i % 2], w_sem.at[i % 2])

        load(0).start()
        for i in range(n_tile):
            if i + 1 < n_tile:
                load(i + 1).start()
            load(i).wait()

            def body(j, carry, i=i):
                vals = p_buf[i % 2, pl.ds(al(j * EW, EW), EW), :].astype(F32)
                inv = lax.rsqrt(jnp.mean(vals * vals, axis=-1, keepdims=True) + NORM_EPS)
                u_buf[pl.ds(al(i * rows + j * EW, EW), EW), :] = (vals * inv * gains[:1, :]).astype(BF16)
                return carry

            lax.fori_loop(0, rows // EW, body, 0)
            if i == n_tile - 2:
                late()

    def tables():
        sign = jnp.where(lax.broadcasted_iota(jnp.int32, (1, HEAD_DIM), 1) < HEAD_DIM // 2, -1.0, 1.0)
        first = pos_ref[0, 0]

        def body(i, carry):
            here = pl.ds(al(i * sub, sub), sub)
            row = first + i * sub + lax.broadcasted_iota(jnp.int32, (sub, HEAD_DIM), 0)
            angle = row.astype(F32) * freq_ref[...]
            cos_ref[here, :] = jnp.cos(angle)
            sin_ref[here, :] = sign * jnp.sin(angle)
            return carry

        lax.fori_loop(0, n_tok // sub, body, 0)
        key = lax.broadcasted_iota(jnp.int32, (1, n_tok), 1)
        bias_ref[...] = jnp.where(key < len_ref[0], 0.0, -jnp.inf)

    def stream(n0, n1, load, compute, hooks={}, lazy=()):
        def fetch(n, slot):
            for cp in load(n, slot):
                cp.start()

        fetch(n0, 0)

        def body(n, carry):
            slot = lax.rem(n - n0, 2)
            late = functools.reduce(jnp.logical_or, [n + 1 == at for at in lazy], n + 1 >= n1)
            pl.when(jnp.logical_not(late))(lambda: fetch(n + 1, 1 - slot))
            for cp in load(n, slot):
                cp.wait()
            compute(n, slot)
            for at, todo in hooks.items():
                @pl.when(n == at)
                def _(at=at, todo=todo):
                    todo()
                    if at + 1 in lazy:
                        fetch(at + 1, 1 - slot)
            return carry

        lax.fori_loop(n0, n1, body, 0)

    def project(hooks, lazy):
        def load(n, slot):
            return (pltpu.make_async_copy(full_p.at[:, pl.ds(al(n * TILE, TILE), TILE)], w_buf.at[slot, :, pl.ds(0, TILE)], w_sem.at[slot]),)

        def compute(n, slot):
            plain = n == 1

            def body(m, carry):
                here = pl.ds(al(m * 2 * rows, rows), 2 * rows)
                acc = jnp.dot(u_buf[here, :], w_buf[slot, :, :TILE], preferred_element_type=F32)
                cos_t = jnp.where(plain, 1.0, cos_ref[here, :])
                sin_t = jnp.where(plain, 0.0, sin_ref[here, :])
                for h in range(TILE // HEAD_DIM):
                    val = acc[:, h * HEAD_DIM:(h + 1) * HEAD_DIM]
                    val = val * cos_t + pltpu.roll(val, HEAD_DIM // 2, 1) * sin_t
                    qkv_buf[here, pl.ds(al(n * TILE + h * HEAD_DIM, HEAD_DIM), HEAD_DIM)] = val.astype(BF16)
                return carry

            lax.fori_loop(0, n_tok // (2 * rows), body, 0)

        stream(0, full_p.shape[1] // TILE, load, compute, hooks, lazy)

    def attend(c, mid=None):
        blk = 2 * sub
        n_blk = rows // blk
        n_old = c * rows
        n_head = q_cols // HEAD_DIM
        per_grp = q_cols // kv_cols
        dims = (((1,), (1,)), ((), ()))
        here = pl.ds(n_old, rows)

        def body(idx, carry):
            head = idx // n_blk
            part = lax.rem(idx, n_blk)
            row0 = al(part * blk, blk)
            col0 = al(head * HEAD_DIM, HEAD_DIM)
            k_at = al((head // per_grp) * HEAD_DIM, HEAD_DIM)
            k_cols, v_cols = pl.ds(k_at, HEAD_DIM), pl.ds(al(kv_cols + k_at, HEAD_DIM), HEAD_DIM)
            q_blk = qkv_buf[pl.ds(al(n_old + row0, blk), blk), pl.ds(al(q_from + col0, HEAD_DIM), HEAD_DIM)]
            s_new = lax.dot_general(q_blk, qkv_buf[here, k_cols], dims, preferred_element_type=F32)
            s_new = s_new * (SCORE_SCALE * LOG2E) + bias_ref[:, here]
            q_idx = row0 + lax.broadcasted_iota(jnp.int32, (blk, rows), 0)
            k_idx = lax.broadcasted_iota(jnp.int32, (blk, rows), 1)
            s_new = jnp.where(k_idx <= q_idx, s_new, -jnp.inf)
            top = jnp.max(s_new, axis=1, keepdims=True)
            if n_old:
                s_old = lax.dot_general(q_blk, qkv_buf[:n_old, k_cols], dims, preferred_element_type=F32)
                s_old = s_old * (SCORE_SCALE * LOG2E) + bias_ref[:, :n_old]
                top = jnp.maximum(top, jnp.max(s_old, axis=1, keepdims=True))
            p_new = jnp.exp2(s_new - top)
            den = jnp.sum(p_new, axis=1, keepdims=True)
            acc = jnp.dot(p_new.astype(BF16), qkv_buf[here, v_cols], preferred_element_type=F32)
            if n_old:
                p_old = jnp.exp2(s_old - top)
                den = den + jnp.sum(p_old, axis=1, keepdims=True)
                acc = acc + jnp.dot(p_old.astype(BF16), qkv_buf[:n_old, v_cols], preferred_element_type=F32)
            out = (acc / den).astype(BF16)
            for s in range(blk // sub):
                dist = lax.rem(part * (blk // sub) + s - me_t + n_tp, n_tp)
                pos = jnp.where(dist == 0, 0, jnp.where(dist == n_tp - 1, 1, dist + 1))
                o_buf[c % 2, pl.ds(al(pos * sub, sub), sub), pl.ds(col0, HEAD_DIM)] = out[s * sub:(s + 1) * sub, :]
            if mid:
                pl.when(idx == n_head)(mid)
            return carry

        lax.fori_loop(0, n_head * n_blk, body, 0)

    def o_place(n):
        depth = wo.shape[0]
        per = width // depth
        return n // per, pl.ds(al(lax.rem(n, per) * depth, depth), depth)

    def o_tile(n):
        slot, here = o_place(n)
        return pltpu.make_async_copy(full_o.at[:, pl.ds(al(n * o_cols, o_cols), o_cols)], w_buf.at[slot, here, :], o_sem.at[n])

    def out_load():
        def body(n, carry):
            o_tile(n).start()
            return carry

        lax.fori_loop(0, n_fsdp, body, 0)

    def out_project(c):
        def body(n, carry):
            if c == 0:
                o_tile(n).wait()
            slot, here = o_place(n)
            acc = jnp.dot(o_buf[c % 2], w_buf[slot, here, :], preferred_element_type=F32)
            p_buf[c % 2, :, pl.ds(al(n * o_cols, o_cols), o_cols)] = acc.astype(BF16)
            return carry

        lax.fori_loop(0, n_fsdp, body, 0)

    def act_copy(c0, nc, n, slot):
        return pltpu.make_async_copy(a_stage.at[slot, pl.ds(0, nc * rows), :],
                                     act.at[pl.ds(c0 * rows, nc * rows), pl.ds(al(n * TILE, TILE), TILE)], a_sem.at[slot])

    def gate_up(pair, n0, n1, hooks={}):
        c0, nc = 2 * pair, 2
        def load(n, slot):
            here = pl.ds(al(n * TILE, TILE), TILE)
            return (pltpu.make_async_copy(full_g.at[:, here], w_buf.at[slot, :, pl.ds(0, TILE)], w_sem.at[slot]),
                    pltpu.make_async_copy(full_u.at[:, here], w_buf.at[slot, :, pl.ds(TILE, TILE)], w_sem.at[2 + slot]))

        def compute(n, slot):
            lhs = u_buf[c0 * rows:(c0 + nc) * rows, :]
            gate = jnp.dot(lhs, w_buf[slot, :, :TILE], preferred_element_type=F32)
            gate = gate * jax.nn.sigmoid(gate)
            val = gate * jnp.dot(lhs, w_buf[slot, :, TILE:], preferred_element_type=F32)

            @pl.when(n - n0 >= 2)
            def _():
                act_copy(c0, nc, n, slot).wait()
            a_stage[slot, :nc * rows, :] = val.astype(BF16)
            act_copy(c0, nc, n, slot).start()

        stream(n0, n1, load, compute, hooks)
        for i in range(min(2, n1 - n0)):
            act_copy(c0, nc, n1 - 1, (n1 - 1 - i - n0) % 2).wait()

    def load_act(pair, start=True):
        c0, nc = 2 * pair, 2
        cp = pltpu.make_async_copy(act.at[pl.ds(c0 * rows, nc * rows), :], u_buf.at[pl.ds(c0 * rows, nc * rows), pl.ds(0, ffn)], l_sem.at[4])
        cp.start() if start else cp.wait()

    def down(k, pair, cs):
        e = N_ROWCH + 2 * k + pair
        slot_p, lane, _ = y_rows(e)
        half = ffn // 2
        row0, n_row = (2 * pair + cs[0]) * rows, len(cs) * rows

        def place(slot, i):
            return pl.ds(0, half), pl.ds(al((2 * slot + i) * TILE, TILE), TILE)

        def load(n, slot):
            return [pltpu.make_async_copy(full_d.at[k, pl.ds(i * half, half), pl.ds(al(n * TILE, TILE), TILE)],
                                          qkv_buf.at[place(slot, i)], wd_sem.at[2 * slot + i]) for i in range(2)]

        def compute(n, slot):
            prod = sum(jnp.dot(u_buf[row0:row0 + n_row, i * half:(i + 1) * half], qkv_buf[place(slot, i)], preferred_element_type=F32)
                       for i in range(2)).astype(BF16)
            for i, ci in enumerate(cs):
                p_buf[slot_p, :, pl.ds(al(lane + ci * c_cols + n * TILE, TILE), TILE)] = prod[i * rows:(i + 1) * rows, :]

        stream(0, c_cols // TILE, load, compute)

    def sent(e):
        for m in (FAR, NEAR, SUM):
            for h in (0, 1):
                y_copy(e, m, h).wait_send()

    def passed(e):
        for h in (0, 1):
            y_copy(e, PASS, h).wait_send()

    def scoped(fn):
        def run(*args, **kw):
            with jax.named_scope("_".join([fn.__name__] + [str(a) for a in args if isinstance(a, int)])):
                return fn(*args, **kw)
        return run

    x_first, x_fwd, x_side, x_third, x_ready = map(scoped, (x_first, x_fwd, x_side, x_third, x_ready))
    y_start, y_add, y_norm, y_final, y_pass, y_ready = map(scoped, (y_start, y_add, y_norm, y_final, y_pass, y_ready))
    norm_rows, project, attend, out_project, gate_up, down = map(scoped, (norm_rows, project, attend, out_project, gate_up, down))
    tables, bounce_in, bounce_out, bounce_end, sent, load_act = map(scoped, (tables, bounce_in, bounce_out, bounce_end, sent, load_act))

    def x_done(*ps):
        x_third(*ps)
        x_ready(*ps)

    def sent_u(*cs):
        for c in cs:
            y_sent_all(c)
            passed(c)

    c0, c1, c2, c3 = range(N_ROWCH)
    units = [N_ROWCH + u for u in unit_at]
    g0, g1, g2, g3 = pg
    d0, d1, d2, d3 = pd
    t0, t1, t2, t3, t4 = GU_SPLIT

    def begin(i):
        if i >= 4:
            sent(units[i - 4])
        parts = ((0,), (1,)) if i == 0 else ((0, 1),)
        for cs in parts:
            down(*unit_list[i], cs)
            y_start(units[i], cs)

    x_first(pk, pv, q0)
    bounce_in(small)
    norm_rows(lambda: x_second(pk, pv))
    bounce_out(small)
    bounce_in(large)
    tables()
    x_fwd(q0)
    x_first(q1)
    x_done(pk, pv)
    bounce_end(small)
    kv_copy = pltpu.make_async_copy(qkv_buf.at[:, pl.ds(0, q_from)], kv_out, r_sem.at[2])

    def have_kv():
        bounce_out(large)
        kv_copy.start()
        x_side(q0)
        x_done(q0)

    project({
        0: lambda: (x_fwd(q1), x_first(*po)),
        1: have_kv,
        3: lambda: (x_side(q1), x_done(q1)),
        4: lambda: (x_second(*po), x_first(*g0, *g1, *g2)),
    }, (2, 4))
    attend(c0)
    x_done(*po)
    out_load()
    bounce_end(large)
    out_project(c0)
    y_start(c0)
    attend(c1)
    out_project(c1)
    y_start(c1)
    x_second(*g0)
    attend(c2, lambda: y_add(c0))
    attend(c3, lambda: y_add(c1))
    x_second(*g1)
    y_norm(c0)
    y_norm(c1)
    sent(c0)
    out_project(c2)
    sent(c1)
    out_project(c3)
    y_pass(c0)
    y_pass(c1)
    y_start(c2)
    y_start(c3)
    x_second(*g2)
    x_first(*g3)
    x_third(*g0)
    x_third(*g1)
    x_ready(*g0)
    y_ready(c0)
    y_ready(c1)
    x_ready(*g1)
    gate_up(0, t0, t3, {t1: lambda: (x_third(*g2), y_add(c2)), t2 - 2: lambda: x_ready(*g2), t2 + 1: lambda: y_add(c3)})
    x_second(*g3)
    x_first(*d0)
    y_norm(c2)
    y_norm(c3)
    x_done(*g3)
    y_pass(c2)
    gate_up(0, t3, t4, {t3 + 1: lambda: (x_second(*d0), x_first(*d1)), t4 - 2: lambda: y_pass(c3)})
    sent_u(c0, c1)
    load_act(0)
    x_done(*d0)
    load_act(0, False)
    kv_copy.wait()
    sent(c2)
    sent(c3)
    begin(0)
    x_second(*d1)
    x_first(*d2)
    y_ready(c2)
    y_ready(c3)
    sent_u(c2, c3)
    f0, f1, f2, f3 = units[:N_DOWN]
    gate_up(1, t0, t4, {
        1: lambda: (y_add(f0), x_done(*d1), begin(1)),
        2: lambda: y_final(*unit_list[0]),
        3: lambda: (x_second(*d2), x_first(*d3)),
        4: lambda: y_add(f1),
        5: lambda: (y_pass(f0), x_third(*d2)),
        6: lambda: (y_final(*unit_list[1]), x_ready(*d2), begin(2)),
        7: lambda: x_second(*d3),
        8: lambda: y_pass(f1),
        9: lambda: (y_add(f2), x_done(*d3), begin(3)),
        10: lambda: y_final(*unit_list[2]),
        12: lambda: y_add(f3),
    })
    load_act(1)
    y_pass(f2)
    load_act(1, False)
    n_unit = len(units)
    half = n_unit // 2
    begin(half)
    y_final(*unit_list[half - 1])
    for i in range(half, n_unit):
        if i + 1 < n_unit:
            begin(i + 1)
        y_add(units[i])
        y_pass(units[i - 1])
        y_final(*unit_list[i])
    y_pass(units[-1])

    for e in units:
        y_ready(e)
        passed(e)
    for e in units[-4:]:
        sent(e)
    for e in units[-2:]:
        y_sent_all(e, (0, 1))
        r_out(e).wait()
    for p in range(len(pieces)):
        for m in range(7):
            x_copy(p, m).wait_send()


def place_kernel(n_tp, n_fsdp, *refs):
    srcs, out_ref = refs[:N_DOWN], refs[N_DOWN]
    sub = srcs[0].shape[2]
    cols = srcs[0].shape[3] // n_fsdp
    for r, dist in enumerate((0, n_tp - 1, 1, 2)):
        here = pl.ds(pl.multiple_of(lax.rem(lax.axis_index("tp") + dist, n_tp) * sub, sub), sub)
        for k in range(N_DOWN):
            for f in range(n_fsdp):
                c0 = (f * N_DOWN + k) * cols
                out_ref[here, c0:c0 + cols] = srcs[k][0, r, :, f * cols:(f + 1) * cols]


def place(res, n_tok, width, n_tp, n_fsdp):
    sub, c_cols = res.shape[2], res.shape[3] // 2

    def src_spec(k):
        return pl.BlockSpec((1, N_REL, sub, c_cols), lambda c: (2 * k + c // 2, 0, 0, c % 2))

    return pl.pallas_call(
        functools.partial(place_kernel, n_tp, n_fsdp),
        out_shape=jax.ShapeDtypeStruct((n_tok, width), BF16),
        grid=(N_ROWCH,),
        in_specs=[src_spec(k) for k in range(N_DOWN)],
        out_specs=pl.BlockSpec((N_REL * sub, width), lambda c: (c, 0)),
        compiler_params=pltpu.CompilerParams(vmem_limit_bytes=VMEM_PLACE),
        name="place",
    )(*([res] * N_DOWN))


def solution(mesh):
    batch_axes = ('dp', 'fsdp')
    n_tp = mesh.shape['tp']
    n_fsdp = mesh.shape['fsdp']
    in_specs = (P(batch_axes, None, None), P(batch_axes, None), P(batch_axes),
                P('fsdp', 'tp'), P('fsdp', 'tp'), P('fsdp', 'tp'), P('tp', 'fsdp'),
                P('fsdp', 'tp'), P('fsdp', 'tp'), P('tp', 'fsdp'), P(None), P(None))
    out_specs = (P(batch_axes, None, None), P(batch_axes, None, 'tp', None), P(batch_axes, None, 'tp', None))

    def local_layer(tokens, positions, valid_len, w_query, w_key, w_value, w_out, w_gate, w_up, w_down, norm_attn, norm_mlp):
        n_tok, width = tokens.shape[1], tokens.shape[2]
        ffn = w_gate.shape[1]
        rows, sub = n_tok // N_ROWCH, n_tok // N_ROWCH // N_REL
        q_cols, kv_cols = w_query.shape[1], w_key.shape[1]
        c_cols = width // N_DOWN
        n_units = 2 * N_DOWN
        freqs = jnp.tile(rope_freqs(), 2)[None]
        gains = jnp.stack([norm_attn, norm_mlp]).astype(F32)
        vm = pl.BlockSpec(memory_space=pltpu.VMEM)
        smem = pl.BlockSpec(memory_space=pltpu.SMEM)
        hbm = pl.BlockSpec(memory_space=pl.ANY)
        n_pieces = 6 + 2 * (len(GU_SPLIT) - 1 + N_DOWN)
        n_y = N_ROWCH + n_units
        st = lambda *s: jax.ShapeDtypeStruct(s, BF16)
        dma = pltpu.SemaphoreType.DMA
        outs = pl.pallas_call(
            functools.partial(layer_kernel, n_tp, n_fsdp),
            out_shape=[st(n_tok, 2 * kv_cols), st(n_units, N_REL, sub, 2 * c_cols),
                       st(width, 2 * kv_cols + q_cols), st(w_out.shape[0], width),
                       st(width, ffn), st(width, ffn), st(N_DOWN, ffn, c_cols), st(n_tok, ffn), st(n_y, 3, sub, width)],
            in_specs=[smem] * 2 + [vm] * 2 + [hbm] * 8,
            out_specs=[hbm] * 9,
            scratch_shapes=[
                pltpu.VMEM((n_tok, width), BF16), pltpu.VMEM((2, width, 2 * TILE), BF16),
                pltpu.VMEM((2, rows, width), BF16),
                pltpu.VMEM((rows, width), BF16), pltpu.VMEM((n_tok, 2 * kv_cols + q_cols), BF16),
                pltpu.VMEM((2, rows, q_cols), BF16), pltpu.VMEM((3, sub, width), BF16),
                pltpu.VMEM((2, sub, 2 * c_cols), BF16), pltpu.VMEM((2, 2 * rows, TILE), BF16),
                pltpu.VMEM((n_tok, HEAD_DIM), F32), pltpu.VMEM((n_tok, HEAD_DIM), F32), pltpu.VMEM((1, n_tok), F32),
                dma((n_pieces, 7)), dma((n_pieces, 7)), dma((n_y, 6, 2)), dma((n_y, 6, 2)),
                dma((4,)), dma((4,)), dma((5,)), dma((2, 11)), dma((2,)), dma((3,)), dma((n_fsdp,)),
            ],
            compiler_params=pltpu.CompilerParams(vmem_limit_bytes=67043328, collective_id=0, has_side_effects=True),
            name="layer",
        )(positions, valid_len, freqs, gains, tokens[0],
          w_key, w_value, w_query, w_out, w_gate, w_up, w_down)
        kv_all, res = outs[0], outs[1]
        hidden = place(res, n_tok, width, n_tp, n_fsdp)
        n_kv = kv_cols // HEAD_DIM
        key_cache = kv_all[:, :kv_cols].reshape(1, n_tok, n_kv, HEAD_DIM)
        value_cache = kv_all[:, kv_cols:].reshape(1, n_tok, n_kv, HEAD_DIM)
        return hidden[None], key_cache, value_cache

    return jax.shard_map(local_layer, mesh=mesh, in_specs=in_specs, out_specs=out_specs, check_vma=False)
```

```python
import functools
import math
import jax
import jax.numpy as jnp
from jax import lax
from jax.experimental import pallas as pl
from jax.experimental.pallas import tpu as pltpu
from jax.sharding import PartitionSpec as P

HEAD_DIM = 128
ROPE_THETA = 500000.0
NORM_EPS = 1e-5
SCORE_SCALE = HEAD_DIM ** -0.5
LOG2E = 1.4426950408889634
BF16 = jnp.bfloat16
F32 = jnp.float32
N_REL = 4
HALVES = (0, 1)
N_ROWCH = 4
N_DOWN = 4
TILE = 256
GU_SPLIT = (0, 2, 6, 10, 14)
MESH = pl.DeviceIdType.MESH
VMEM_PLACE = 67043328


def rope_freqs():
    half_idx = jnp.arange(HEAD_DIM // 2, dtype=F32)
    inv_freq = jnp.power(ROPE_THETA, -2.0 * half_idx / HEAD_DIM)
    wave_len = 2.0 * math.pi / inv_freq
    smooth = (8192.0 / wave_len - 1.0) / 3.0
    blended = (1.0 - smooth) * inv_freq / 8.0 + smooth * inv_freq
    return jnp.where(wave_len < 2048.0, inv_freq, jnp.where(wave_len > 8192.0, inv_freq / 8.0, blended))


def upto(n):
    return pl.ds(0, n)


def layer_kernel(n_tp, n_fsdp, *refs):
    (pos_ref, len_ref, freq_ref, gain_a, gain_m, tok, wk, wv, wq, wo, wg, wu, wd,
     kv_out, res, full_p, full_o, full_g, full_u, full_d, act, rs,
     u_buf, w_buf, p_buf, x1_buf, qkv_buf, o_buf, stage, r_buf, a_stage, cos_ref, sin_ref, bias_ref, gains,
     x_send, x_recv, y_send, y_recv, w_sem, wd_sem, l_sem, b_sem, a_sem, r_sem, o_sem) = refs
    n_tok, width = tok.shape
    rows = n_tok // N_ROWCH
    sub = rows // N_REL
    k_rows = wk.shape[0]
    kv_cols = wk.shape[1]
    q_cols = wq.shape[1]
    ffn = wg.shape[1]
    o_cols = wo.shape[1]
    d_cols = wd.shape[1] // N_DOWN
    c_cols = d_cols * n_fsdp
    n_x = n_fsdp // 2

    me_t = lax.axis_index("tp")
    me_f = lax.axis_index("fsdp")
    chip, core = me_f // 2, me_f % 2
    t_right = lax.rem(me_t + 1, n_tp)
    t_left = lax.rem(me_t + n_tp - 1, n_tp)
    f_right = 2 * lax.rem(chip + 1, n_x) + core
    f_left = 2 * lax.rem(chip + n_x - 1, n_x) + core
    f_far = 2 * lax.rem(chip + 2, n_x) + core
    other = 1 - 2 * core
    f_twin = me_f + other

    barrier = pltpu.get_barrier_semaphore()
    for peer in ({"tp": t_left}, {"tp": t_right}, {"fsdp": f_left}, {"fsdp": f_right}, {"fsdp": f_twin}):
        pl.semaphore_signal(barrier, inc=1, device_id=peer, device_id_type=MESH)
    pl.semaphore_wait(barrier, 5)

    def al(val, mult):
        return pl.multiple_of(val, mult)

    groups = []

    def add_group(pieces, area):
        groups.append((pieces, area))
        return len(groups) - 1

    def by_rows(full, c0, n):
        return lambda f: full.at[pl.ds(al(f * k_rows, k_rows), k_rows), pl.ds(c0, n)]

    def halves(own, place):
        n = own.shape[0] // 2
        return [(own.at[pl.ds(i * n, n), :], lambda f, i=i: place(f).at[pl.ds(i * n, n), :], i) for i in HALVES]

    def o_piece(f):
        return full_o.at[:, pl.ds(al(f * o_cols, o_cols), o_cols)]

    def d_piece(k, f):
        return full_d.at[k, :, pl.ds(al(f * d_cols, d_cols), d_cols)]

    half_q = q_cols // 2
    q_from = 2 * kv_cols

    def row_area(full, c0, cols):
        return lambda n: full.at[upto(n * k_rows), pl.ds(c0, cols)]

    pkv = add_group([(own, by_rows(full_p, i * kv_cols, kv_cols), i) for i, own in enumerate((wk, wv))], row_area(full_p, 0, q_from))
    q0, q1 = [add_group([(wq.at[:, pl.ds(i * half_q, half_q)], by_rows(full_p, q_from + i * half_q, half_q), i)],
                        row_area(full_p, q_from + i * half_q, half_q)) for i in HALVES]
    po = add_group(halves(wo, o_piece), lambda n: full_o.at[:, upto(n * o_cols)])
    g0, g1, g2, g3 = [
        add_group([(own.at[:, pl.ds(lo * TILE, (hi - lo) * TILE)], by_rows(full, lo * TILE, (hi - lo) * TILE), i)
                   for i, (own, full) in enumerate(((wg, full_g), (wu, full_u)))], row_area(full_g, 0, 2 * (hi - lo) * TILE))
        for lo, hi in zip(GU_SPLIT, GU_SPLIT[1:])]
    d0, d1, d2, d3 = [
        add_group(halves(wd.at[:, pl.ds(k * d_cols, d_cols)], functools.partial(d_piece, k)), lambda n, k=k: full_d.at[k, :, upto(n * d_cols)])
        for k in range(N_DOWN)]

    FIRST, FAR_ON, TWIN = HALVES, 2, 3

    def x_copy(g, i, m):
        own, place, way = groups[g][0][i]
        near = (f_left, f_right)
        if m in FIRST:
            src, owner, target = own, me_f, near[1 - m]
        elif m == FAR_ON:
            owner, target = near[way], near[1 - way]
            src = place(owner)
        else:
            owner, target = (me_f, f_left, f_right, f_far)[m - TWIN], f_twin
            src = own if m == TWIN else place(owner)
        return pltpu.make_async_remote_copy(src_ref=src, dst_ref=place(owner), send_sem=x_send.at[g], recv_sem=x_recv.at[g, min(m, TWIN)],
                                            device_id={"fsdp": target}, device_id_type=MESH)

    def x_all(g, *ms):
        for m in ms:
            for i in range(len(groups[g][0])):
                x_copy(g, i, m).start()

    def x_taken(g, kind, n=1):
        area = groups[g][1](n)
        return pltpu.make_async_remote_copy(src_ref=area, dst_ref=area, send_sem=x_send.at[g], recv_sem=x_recv.at[g, kind],
                                            device_id={"fsdp": f_twin}, device_id_type=MESH)

    def x_first(*gs):
        for g in gs:
            x_all(g, *FIRST, TWIN)

    def x_fwd(g):
        for i, piece in enumerate(groups[g][0]):
            x_taken(g, piece[2]).wait_recv()
            x_copy(g, i, FAR_ON).start()

    def x_side(g):
        if len(groups[g][0]) == 1:
            x_taken(g, 1 - groups[g][0][0][2]).wait_recv()
        x_all(g, TWIN + 1, TWIN + 2)

    def x_second(g):
        x_fwd(g)
        x_side(g)

    def x_third(g):
        x_taken(g, FAR_ON).wait_recv()
        x_all(g, TWIN + 3)

    def x_ready(g):
        x_taken(g, TWIN, 4).wait_recv()

    def x_sent(*gs):
        for g in gs:
            x_taken(g, TWIN, 7).wait_send()

    unit_list = [(k, pair) for pair in range(2) for k in range(N_DOWN)]
    unit_at = [2 * k + pair for k, pair in unit_list]
    unit_order = {u: i for i, u in enumerate(unit_at)}

    def y_rows(e):
        if e < N_ROWCH:
            slot, lane, wid = e % 2, 0, width
        else:
            q = unit_order[e - N_ROWCH] % 4
            slot, lane, wid = q // 2, (q % 2) * (width // 2), 2 * c_cols
        return slot, lane, wid

    def lanes(e, h):
        slot, lane, wid = y_rows(e)
        return slot, pl.ds(lane + h * (wid // 2), wid // 2), pl.ds(h * (wid // 2), wid // 2)

    def g_slice(e, r):
        if e < N_ROWCH:
            return u_buf.at[pl.ds(e * rows + r * sub, sub), :]
        return res.at[e - N_ROWCH, r]

    FAR, NEAR, SUM, RIGHT, LEFT, PASS = range(6)
    OUT, SPREAD, ON = range(3)
    sent_as = (OUT, OUT, OUT, SPREAD, SPREAD, ON)
    GOT_FAR, GOT_SUMS, GOT_SPREAD, GOT_REST = range(4)

    def got_as(e, m, h):
        if m in (RIGHT, LEFT):
            return GOT_SPREAD if e < N_ROWCH or m == LEFT - h else GOT_REST
        return {FAR: GOT_FAR, PASS: GOT_REST}.get(m, GOT_SUMS)

    def y_taken(e, kind, n):
        area = rs.at[e, upto(n), :, upto(y_rows(e)[2])]
        return pltpu.make_async_remote_copy(src_ref=area, dst_ref=area, send_sem=y_send.at[e, min(kind, ON)], recv_sem=y_recv.at[e, kind],
                                            device_id={"tp": t_right}, device_id_type=MESH)

    def y_copy(e, m, h=0):
        slot, here, there = lanes(e, h)
        if m in (RIGHT, LEFT):
            src, dst, to = g_slice(e, 0), g_slice(e, m - 2), m - 3
            if e >= N_ROWCH:
                src, dst = r_buf.at[unit_order[e - N_ROWCH] % 2, :, there], dst.at[:, there]
        elif m == PASS:
            src, dst, to = g_slice(e, 2 - h).at[:, there], g_slice(e, 3).at[:, there], 1 - h
        else:
            r, i, to = {FAR: (3, 0, h), NEAR: (1 + h, 2 - h, 1 - h), SUM: (2 - h, 1 + h, h)}[m]
            src, dst = p_buf.at[slot, pl.ds(r * sub, sub), here], rs.at[e, i, :, there]
        return pltpu.make_async_remote_copy(src_ref=src, dst_ref=dst, send_sem=y_send.at[e, sent_as[m]], recv_sem=y_recv.at[e, got_as(e, m, h)],
                                            device_id={"tp": t_right if to == 0 else t_left}, device_id_type=MESH)

    def rs_slice(e, i):
        return rs.at[e, i, :, upto(y_rows(e)[2])]

    def load_stage(e, idx):
        wid = y_rows(e)[2]
        for i in idx:
            pltpu.make_async_copy(rs_slice(e, i), stage.at[i, :, upto(wid)], l_sem.at[i]).start()

    def wait_stage(e, idx):
        wid = y_rows(e)[2]
        for i in idx:
            pltpu.make_async_copy(rs_slice(e, i), stage.at[i, :, upto(wid)], l_sem.at[i]).wait()

    def y_start(e, hs=HALVES):
        for m in (FAR, NEAR):
            for h in hs:
                y_copy(e, m, h).start()

    def y_have(e):
        y_taken(e, GOT_SUMS, 2).wait_recv()

    def y_send_all(e, h=0):
        y_copy(e, LEFT, h).start()
        y_copy(e, RIGHT, h).start()

    def y_sent_all(e):
        y_taken(e, SPREAD, 2).wait_send()

    EW = 32

    def y_add(e):
        y_taken(e, GOT_FAR, 1).wait_recv()
        for h in HALVES:
            there = lanes(e, h)[2]
            pltpu.make_async_copy(rs.at[e, 0, :, there], stage.at[0, :, there], l_sem.at[h]).start()
        for h in HALVES:
            slot, here, there = lanes(e, h)
            pltpu.make_async_copy(rs.at[e, 0, :, there], stage.at[0, :, there], l_sem.at[h]).wait()

            def body(i, carry, h=h, here=here, there=there):
                rr = pl.ds(al((2 - h) * sub + i * EW, EW), EW)
                tot = p_buf[slot, rr, here].astype(F32) + stage[0, pl.ds(al(i * EW, EW), EW), there].astype(F32)
                p_buf[slot, rr, here] = tot.astype(BF16)
                return carry

            lax.fori_loop(0, sub // EW, body, 0)
            y_copy(e, SUM, h).start()

    def tok_copy(c):
        row0 = al(c * rows + me_t * sub, sub)
        return pltpu.make_async_copy(tok.at[pl.ds(row0, sub), :], stage.at[0], l_sem.at[3])

    def y_norm(c):
        slot = c % 2
        tok_copy(c).start()
        y_have(c)
        load_stage(c, (1, 2))
        wait_stage(c, (1, 2))
        tok_copy(c).wait()

        def body(i, carry):
            rr = al(i * EW, EW)
            here = pl.ds(rr, EW)
            tot = p_buf[slot, here, :].astype(F32) + stage[1, here, :].astype(F32) + stage[2, here, :].astype(F32)
            x1 = (stage[0, here, :].astype(F32) + tot).astype(BF16)
            x1_buf[pl.ds(al(c * sub + i * EW, EW), EW), :] = x1
            xf = x1.astype(F32)
            inv = lax.rsqrt(jnp.mean(xf * xf, axis=-1, keepdims=True) + NORM_EPS)
            u_buf[pl.ds(al(c * rows + i * EW, EW), EW), :] = (xf * inv * gains[1:, :]).astype(BF16)
            return carry

        lax.fori_loop(0, sub // EW, body, 0)
        y_send_all(c)

    def y_final(k, pair):
        unit = 2 * k + pair
        e = N_ROWCH + unit
        r_slot = unit_order[unit] % 2
        if unit_order[unit] >= 2:
            before = N_ROWCH + unit_at[unit_order[unit] - 2]
            y_sent_all(before)
            r_out(before).wait()
        y_have(e)
        loads = [[pltpu.make_async_copy(rs.at[e, i, :, lanes(e, h)[2]], stage.at[i, :, lanes(e, h)[2]], l_sem.at[2 * h + i - 1])
                  for i in (1, 2)] for h in HALVES]
        for cp in loads[0] + loads[1]:
            cp.start()
        for h in HALVES:
            slot, mine, there = lanes(e, h)
            for cp in loads[h]:
                cp.wait()

            def body(i, carry, h=h, slot=slot, mine=mine):
                here = pl.ds(al(i * EW, EW), EW)
                x_rows = pl.ds(al((2 * pair + h) * sub + i * EW, EW), EW)
                for f in range(n_fsdp):
                    at = pl.ds(h * c_cols + f * d_cols, d_cols)
                    tot = (p_buf[slot, here, pl.ds(mine.start + f * d_cols, d_cols)].astype(F32)
                           + stage[1, here, at].astype(F32) + stage[2, here, at].astype(F32))
                    x1 = x1_buf[x_rows, pl.ds((f * N_DOWN + k) * d_cols, d_cols)].astype(F32)
                    r_buf[r_slot, here, at] = (x1 + tot).astype(BF16)
                return carry

            lax.fori_loop(0, sub // EW, body, 0)
            y_send_all(e, h)
        r_out(e).start()

    def r_out(e):
        return pltpu.make_async_copy(r_buf.at[unit_order[e - N_ROWCH] % 2], res.at[e - N_ROWCH, 0], r_sem.at[unit_order[e - N_ROWCH] % 2])

    def y_pass(e):
        y_taken(e, GOT_SPREAD, 2 if e < N_ROWCH else 1).wait_recv()
        for h in HALVES:
            y_copy(e, PASS, h).start()

    def y_ready(e):
        y_taken(e, GOT_REST, 1 if e < N_ROWCH else 2).wait_recv()

    def bounce(src, via, dst, i):
        return pltpu.make_async_copy(src, via, b_sem.at[0, i]), pltpu.make_async_copy(via, dst, b_sem.at[1, i])

    small = [
        bounce(wk, w_buf.at[0, upto(k_rows), upto(kv_cols)], by_rows(full_p, 0, kv_cols)(me_f), 0),
        bounce(wv, w_buf.at[0, upto(k_rows), pl.ds(kv_cols, kv_cols)], by_rows(full_p, kv_cols, kv_cols)(me_f), 1),
        bounce(wq.at[:, upto(half_q)], w_buf.at[0, pl.ds(k_rows, k_rows), :], by_rows(full_p, q_from, half_q)(me_f), 2),
        bounce(wq.at[:, pl.ds(half_q, half_q)], w_buf.at[0, pl.ds(2 * k_rows, k_rows), :], by_rows(full_p, q_from + half_q, half_q)(me_f), 3),
        bounce(wo, w_buf.at[0, pl.ds(3 * k_rows, wo.shape[0]), :], o_piece(me_f), 4),
    ] + [
        bounce(wd.at[:, pl.ds(k * d_cols, d_cols)], w_buf.at[1, upto(ffn), pl.ds(k * d_cols, d_cols)], d_piece(k, me_f), 5 + k)
        for k in range(N_DOWN)
    ]
    large = [
        bounce(wg, p_buf.at[0, :, upto(ffn)], by_rows(full_g, 0, ffn)(me_f), 9),
        bounce(wu, p_buf.at[1, :, upto(ffn)], by_rows(full_u, 0, ffn)(me_f), 10),
    ]

    def bounce_in(group):
        for a, _ in group:
            a.start()

    def bounce_out(group):
        for a, b in group:
            a.wait()
            b.start()

    def bounce_end(group):
        for _, b in group:
            b.wait()

    def norm_rows(late):
        n_tile = n_tok // rows

        def load(i):
            return pltpu.make_async_copy(tok.at[pl.ds(i * rows, rows), :], p_buf.at[i % 2], w_sem.at[i % 2])

        load(0).start()
        for i in range(n_tile):
            if i + 1 < n_tile:
                load(i + 1).start()
            load(i).wait()

            def body(j, carry, i=i):
                vals = p_buf[i % 2, pl.ds(al(j * EW, EW), EW), :].astype(F32)
                inv = lax.rsqrt(jnp.mean(vals * vals, axis=-1, keepdims=True) + NORM_EPS)
                u_buf[pl.ds(al(i * rows + j * EW, EW), EW), :] = (vals * inv * gains[:1, :]).astype(BF16)
                return carry

            lax.fori_loop(0, rows // EW, body, 0)
            if i == n_tile - 2:
                late()

    def tables():
        sign = jnp.where(lax.broadcasted_iota(jnp.int32, (1, HEAD_DIM), 1) < HEAD_DIM // 2, -1.0, 1.0)
        first = pos_ref[0, 0]

        def body(i, carry):
            here = pl.ds(al(i * sub, sub), sub)
            row = first + i * sub + lax.broadcasted_iota(jnp.int32, (sub, HEAD_DIM), 0)
            angle = row.astype(F32) * freq_ref[...]
            cos_ref[here, :] = jnp.cos(angle)
            sin_ref[here, :] = sign * jnp.sin(angle)
            return carry

        lax.fori_loop(0, n_tok // sub, body, 0)
        key = lax.broadcasted_iota(jnp.int32, (1, n_tok), 1)
        bias_ref[...] = jnp.where(key < len_ref[0], 0.0, -jnp.inf)

    def stream(n0, n1, load, compute, hooks={}, lazy=(), fetched=False, then=None):
        def fetch(n, slot):
            for cp in load(n, slot):
                cp.start()

        if not fetched:
            fetch(n0, 0)

        def body(n, carry):
            slot = lax.rem(n - n0, 2)
            late = functools.reduce(jnp.logical_or, [n + 1 == at for at in lazy], n + 1 >= n1)
            pl.when(jnp.logical_not(late))(lambda: fetch(n + 1, 1 - slot))
            if then:
                pl.when(n + 1 == n1)(then)
            for cp in load(n, slot):
                cp.wait()
            compute(n, slot)
            for at, todo in hooks.items():
                @pl.when(n == at)
                def _(at=at, todo=todo):
                    todo()
                    if at + 1 in lazy:
                        fetch(at + 1, 1 - slot)
            return carry

        lax.fori_loop(n0, n1, body, 0)

    def project(hooks, lazy):
        def load(n, slot):
            return (pltpu.make_async_copy(full_p.at[:, pl.ds(al(n * TILE, TILE), TILE)], w_buf.at[slot, :, upto(TILE)], w_sem.at[slot]),)

        def compute(n, slot):
            plain = n == 1

            def body(m, carry):
                here = pl.ds(al(m * 2 * rows, rows), 2 * rows)
                acc = jnp.dot(u_buf[here, :], w_buf[slot, :, :TILE], preferred_element_type=F32)
                cos_t = jnp.where(plain, 1.0, cos_ref[here, :])
                sin_t = jnp.where(plain, 0.0, sin_ref[here, :])
                for h in range(TILE // HEAD_DIM):
                    val = acc[:, h * HEAD_DIM:(h + 1) * HEAD_DIM]
                    val = val * cos_t + pltpu.roll(val, HEAD_DIM // 2, 1) * sin_t
                    qkv_buf[here, pl.ds(al(n * TILE + h * HEAD_DIM, HEAD_DIM), HEAD_DIM)] = val.astype(BF16)
                return carry

            lax.fori_loop(0, n_tok // (2 * rows), body, 0)

        stream(0, full_p.shape[1] // TILE, load, compute, hooks, lazy)

    def attend(c, mid=None):
        blk = 2 * sub
        n_blk = rows // blk
        n_old = c * rows
        n_head = q_cols // HEAD_DIM
        per_grp = q_cols // kv_cols
        dims = (((1,), (1,)), ((), ()))
        here = pl.ds(n_old, rows)

        def body(idx, carry):
            head = idx // n_blk
            part = lax.rem(idx, n_blk)
            row0 = al(part * blk, blk)
            col0 = al(head * HEAD_DIM, HEAD_DIM)
            k_at = al((head // per_grp) * HEAD_DIM, HEAD_DIM)
            k_cols, v_cols = pl.ds(k_at, HEAD_DIM), pl.ds(al(kv_cols + k_at, HEAD_DIM), HEAD_DIM)
            q_blk = qkv_buf[pl.ds(al(n_old + row0, blk), blk), pl.ds(al(q_from + col0, HEAD_DIM), HEAD_DIM)]
            s_new = lax.dot_general(q_blk, qkv_buf[here, k_cols], dims, preferred_element_type=F32)
            s_new = s_new * (SCORE_SCALE * LOG2E) + bias_ref[:, here]
            q_idx = row0 + lax.broadcasted_iota(jnp.int32, (blk, rows), 0)
            k_idx = lax.broadcasted_iota(jnp.int32, (blk, rows), 1)
            s_new = jnp.where(k_idx <= q_idx, s_new, -jnp.inf)
            top = jnp.max(s_new, axis=1, keepdims=True)
            if n_old:
                s_old = lax.dot_general(q_blk, qkv_buf[:n_old, k_cols], dims, preferred_element_type=F32)
                s_old = s_old * (SCORE_SCALE * LOG2E) + bias_ref[:, :n_old]
                top = jnp.maximum(top, jnp.max(s_old, axis=1, keepdims=True))
            p_new = jnp.exp2(s_new - top)
            den = jnp.sum(p_new, axis=1, keepdims=True)
            acc = jnp.dot(p_new.astype(BF16), qkv_buf[here, v_cols], preferred_element_type=F32)
            if n_old:
                p_old = jnp.exp2(s_old - top)
                den = den + jnp.sum(p_old, axis=1, keepdims=True)
                acc = acc + jnp.dot(p_old.astype(BF16), qkv_buf[:n_old, v_cols], preferred_element_type=F32)
            out = (acc / den).astype(BF16)
            for s in range(blk // sub):
                dist = lax.rem(part * (blk // sub) + s - me_t + n_tp, n_tp)
                pos = jnp.where(dist == 0, 0, jnp.where(dist == n_tp - 1, 1, dist + 1))
                o_buf[c % 2, pl.ds(al(pos * sub, sub), sub), pl.ds(col0, HEAD_DIM)] = out[s * sub:(s + 1) * sub, :]
            if mid:
                pl.when(idx == n_head)(mid)
            return carry

        lax.fori_loop(0, n_head * n_blk, body, 0)

    def o_place(n):
        depth = wo.shape[0]
        per = width // depth
        return n // per, pl.ds(al(lax.rem(n, per) * depth, depth), depth)

    def o_tile(n):
        slot, here = o_place(n)
        return pltpu.make_async_copy(full_o.at[:, pl.ds(al(n * o_cols, o_cols), o_cols)], w_buf.at[slot, here, :], o_sem.at[n])

    def out_load():
        def body(n, carry):
            o_tile(n).start()
            return carry

        lax.fori_loop(0, n_fsdp, body, 0)

    def out_project(c):
        def body(n, carry):
            if c == 0:
                o_tile(n).wait()
            slot, here = o_place(n)
            acc = jnp.dot(o_buf[c % 2], w_buf[slot, here, :], preferred_element_type=F32)
            p_buf[c % 2, :, pl.ds(al(n * o_cols, o_cols), o_cols)] = acc.astype(BF16)
            return carry

        lax.fori_loop(0, n_fsdp, body, 0)

    def act_copy(c0, nc, n, slot):
        return pltpu.make_async_copy(a_stage.at[slot, upto(nc * rows), :],
                                     act.at[pl.ds(c0 * rows, nc * rows), pl.ds(al(n * TILE, TILE), TILE)], a_sem.at[slot])

    def gate_up(pair, n0, n1, hooks={}):
        c0, nc = 2 * pair, 2
        def load(n, slot):
            here = pl.ds(al(n * TILE, TILE), TILE)
            return (pltpu.make_async_copy(full_g.at[:, here], w_buf.at[slot, :, upto(TILE)], w_sem.at[slot]),
                    pltpu.make_async_copy(full_u.at[:, here], w_buf.at[slot, :, pl.ds(TILE, TILE)], w_sem.at[2 + slot]))

        def compute(n, slot):
            lhs = u_buf[c0 * rows:(c0 + nc) * rows, :]
            gate = jnp.dot(lhs, w_buf[slot, :, :TILE], preferred_element_type=F32)
            gate = gate * jax.nn.sigmoid(gate)
            val = gate * jnp.dot(lhs, w_buf[slot, :, TILE:], preferred_element_type=F32)

            @pl.when(n - n0 >= 2)
            def _():
                act_copy(c0, nc, n, slot).wait()
            a_stage[slot, :nc * rows, :] = val.astype(BF16)
            act_copy(c0, nc, n, slot).start()

        stream(n0, n1, load, compute, hooks)
        for i in range(min(2, n1 - n0)):
            act_copy(c0, nc, n1 - 1, (n1 - 1 - i - n0) % 2).wait()

    def load_act(c):
        here = pl.ds(c * rows, rows)
        return pltpu.make_async_copy(act.at[here, :], u_buf.at[here, upto(ffn)], r_sem.at[3 + c % 2])

    def down_place(slot, i):
        return upto(ffn // 2), pl.ds(al((2 * slot + i) * TILE, TILE), TILE)

    def down_tile(k, n, slot):
        return [pltpu.make_async_copy(full_d.at[k, pl.ds(i * (ffn // 2), ffn // 2), pl.ds(al(n * TILE, TILE), TILE)],
                                      qkv_buf.at[down_place(slot, i)], wd_sem.at[2 * slot + i]) for i in HALVES]

    def down_fetch(k):
        for cp in down_tile(k, 0, 0):
            cp.start()

    def down(k, pair, cs, fetched, then):
        e = N_ROWCH + 2 * k + pair
        slot_p, lane, _ = y_rows(e)
        half = ffn // 2
        row0, n_row = (2 * pair + cs[0]) * rows, len(cs) * rows

        def compute(n, slot):
            prod = sum(jnp.dot(u_buf[row0:row0 + n_row, i * half:(i + 1) * half], qkv_buf[down_place(slot, i)], preferred_element_type=F32)
                       for i in HALVES).astype(BF16)
            for i, ci in enumerate(cs):
                p_buf[slot_p, :, pl.ds(al(lane + ci * c_cols + n * TILE, TILE), TILE)] = prod[i * rows:(i + 1) * rows, :]

        stream(0, c_cols // TILE, functools.partial(down_tile, k), compute, fetched=fetched, then=then)

    def sent(e):
        y_taken(e, OUT, 3).wait_send()

    def passed(e):
        y_taken(e, ON, 1).wait_send()

    def scoped(fn):
        def run(*args, **kw):
            with jax.named_scope("_".join([fn.__name__] + [str(a) for a in args if isinstance(a, int)])):
                return fn(*args, **kw)
        return run

    x_first, x_fwd, x_side, x_third, x_ready = map(scoped, (x_first, x_fwd, x_side, x_third, x_ready))
    y_start, y_add, y_norm, y_final, y_pass, y_ready = map(scoped, (y_start, y_add, y_norm, y_final, y_pass, y_ready))
    norm_rows, project, attend, out_project, gate_up, down = map(scoped, (norm_rows, project, attend, out_project, gate_up, down))
    tables, bounce_in, bounce_out, bounce_end, sent = map(scoped, (tables, bounce_in, bounce_out, bounce_end, sent))

    def x_done(g):
        x_third(g)
        x_ready(g)

    def sent_u(*cs):
        for c in cs:
            y_sent_all(c)
            passed(c)

    c0, c1, c2, c3 = range(N_ROWCH)
    units = [N_ROWCH + u for u in unit_at]
    t0, t1, t2, t3, t4 = GU_SPLIT

    def begin(i, fetched=False, ahead=False, wait=None):
        if i >= 4:
            sent(units[i - 4])
        k, pair = unit_list[i]
        parts = [(h,) for h in HALVES] if wait else (HALVES,)
        for cs in parts:
            last = cs == parts[-1]
            then = functools.partial(down_fetch, unit_list[i + 1][0]) if last and ahead else None if last else functools.partial(down_fetch, k)
            if wait:
                wait(cs[0])
            down(k, pair, cs, fetched or cs != parts[0], then)
            y_start(units[i], cs)

    x_first(pkv, q0)
    bounce_in(small)
    gains[:1, :] = gain_a[...].astype(F32)[None]
    gains[1:, :] = gain_m[...].astype(F32)[None]
    norm_rows(lambda: x_second(pkv))
    bounce_out(small)
    bounce_in(large)
    tables()
    x_fwd(q0)
    x_first(q1)
    x_done(pkv)
    bounce_end(small)
    kv_copy = pltpu.make_async_copy(qkv_buf.at[:, upto(q_from)], kv_out, r_sem.at[2])

    def have_kv():
        bounce_out(large)
        kv_copy.start()
        x_side(q0)
        x_done(q0)

    project({
        0: lambda: (x_fwd(q1), x_first(po)),
        1: have_kv,
        3: lambda: (x_side(q1), x_done(q1)),
        4: lambda: (x_second(po), x_first(g0, g1, g2)),
    }, (2, 4))
    attend(c0)
    x_done(po)
    out_load()
    bounce_end(large)
    out_project(c0)
    y_start(c0)
    attend(c1)
    out_project(c1)
    y_start(c1)
    x_second(g0)
    attend(c2, lambda: y_add(c0))
    attend(c3, lambda: y_add(c1))
    x_second(g1)
    y_norm(c0)
    y_norm(c1)
    sent(c0)
    out_project(c2)
    sent(c1)
    out_project(c3)
    y_pass(c0)
    y_pass(c1)
    y_start(c2)
    y_start(c3)
    x_second(g2)
    x_first(g3)
    x_third(g0)
    x_third(g1)
    x_ready(g0)
    y_ready(c0)
    y_ready(c1)
    x_ready(g1)
    gate_up(0, t0, t3, {t1: lambda: (x_third(g2), y_add(c2)), t2 - 2: lambda: x_ready(g2), t2 + 1: lambda: y_add(c3)})
    x_second(g3)
    x_first(d0)
    y_norm(c2)
    y_norm(c3)
    x_done(g3)
    y_pass(c2)
    gate_up(0, t3, t4, {t3 + 1: lambda: (x_second(d0), x_first(d1)), t4 - 2: lambda: y_pass(c3)})
    sent_u(c0, c1)
    load_act(c0).start()
    load_act(c1).start()
    kv_copy.wait()
    x_done(d0)
    down_fetch(0)
    sent(c2)
    sent(c3)
    (load_act(c0).wait(), load_act(c1).wait(), begin(0, True))
    x_second(d1)
    x_first(d2)
    y_ready(c2)
    y_ready(c3)
    sent_u(c2, c3)
    f0, f1, f2, f3 = units[:N_DOWN]
    gate_up(1, t0, t4, {
        1: lambda: (y_add(f0), x_done(d1), begin(1)),
        2: lambda: y_final(*unit_list[0]),
        3: lambda: (x_second(d2), x_first(d3)),
        4: lambda: y_add(f1),
        5: lambda: (y_pass(f0), x_third(d2)),
        6: lambda: (y_final(*unit_list[1]), x_ready(d2), begin(2)),
        7: lambda: x_second(d3),
        8: lambda: y_pass(f1),
        9: lambda: (y_add(f2), x_done(d3), begin(3)),
        10: lambda: y_final(*unit_list[2]),
        12: lambda: (y_add(f3), down_fetch(0)),
    })
    load_act(c2).start()
    load_act(c3).start()
    y_pass(f2)
    n_unit = len(units)
    half = n_unit // 2
    begin(half, True, True, lambda h: load_act(2 + h).wait())
    y_final(*unit_list[half - 1])
    for i in range(half, n_unit):
        if i + 1 < n_unit:
            begin(i + 1, True, i + 2 < n_unit)
        y_add(units[i])
        x_sent(*range(len(groups) * (i - half) // half, len(groups) * (i + 1 - half) // half))
        y_pass(units[i - 1])
        if i > half:
            y_ready(units[i - 2])
            passed(units[i - 2])
        y_final(*unit_list[i])
    for e in units[-4:]:
        sent(e)
    y_pass(units[-1])
    for e in units[:half - 1] + units[-2:]:
        y_ready(e)
        passed(e)
    for e in units[-2:]:
        y_sent_all(e)
        r_out(e).wait()


def place_kernel(n_tp, n_fsdp, *refs):
    srcs, kv_ref = refs[:N_DOWN], refs[N_DOWN]
    out_ref, *cache_refs = refs[N_DOWN + 1:]
    for i, cache in enumerate(cache_refs):
        cols = cache.shape[1] * cache.shape[2]
        cache[...] = kv_ref[:, i * cols:(i + 1) * cols].reshape(cache.shape)
    sub = srcs[0].shape[2]
    cols = srcs[0].shape[3] // n_fsdp
    for r, dist in enumerate((0, n_tp - 1, 1, 2)):
        here = pl.ds(pl.multiple_of(lax.rem(lax.axis_index("tp") + dist, n_tp) * sub, sub), sub)
        for k in range(N_DOWN):
            for f in range(n_fsdp):
                c0 = (f * N_DOWN + k) * cols
                out_ref[here, c0:c0 + cols] = srcs[k][0, r, :, f * cols:(f + 1) * cols]


def place(res, kv_all, n_tok, width, n_tp, n_fsdp):
    rows, kv_cols = n_tok // N_ROWCH, kv_all.shape[1]
    n_kv = kv_cols // 2 // HEAD_DIM
    cache = jax.ShapeDtypeStruct((n_tok, n_kv, HEAD_DIM), BF16)
    sub, c_cols = res.shape[2], res.shape[3] // 2

    def src_spec(k):
        return pl.BlockSpec((1, N_REL, sub, c_cols), lambda c: (2 * k + c // 2, 0, 0, c % 2))

    return pl.pallas_call(
        functools.partial(place_kernel, n_tp, n_fsdp),
        out_shape=[jax.ShapeDtypeStruct((n_tok, width), BF16), cache, cache],
        grid=(N_ROWCH,),
        in_specs=[src_spec(k) for k in range(N_DOWN)] + [pl.BlockSpec((rows, kv_cols), lambda c: (c, 0))],
        out_specs=[pl.BlockSpec((rows, width), lambda c: (c, 0))] + [pl.BlockSpec((rows, n_kv, HEAD_DIM), lambda c: (c, 0, 0))] * 2,
        compiler_params=pltpu.CompilerParams(vmem_limit_bytes=VMEM_PLACE),
        name="place",
    )(*([res] * N_DOWN), kv_all)


def solution(mesh):
    batch_axes = ('dp', 'fsdp')
    n_tp = mesh.shape['tp']
    n_fsdp = mesh.shape['fsdp']
    in_specs = (P(batch_axes, None, None), P(batch_axes, None), P(batch_axes),
                P('fsdp', 'tp'), P('fsdp', 'tp'), P('fsdp', 'tp'), P('tp', 'fsdp'),
                P('fsdp', 'tp'), P('fsdp', 'tp'), P('tp', 'fsdp'), P(None), P(None))
    out_specs = (P(batch_axes, None, None), P(batch_axes, None, 'tp', None), P(batch_axes, None, 'tp', None))

    def local_layer(tokens, positions, valid_len, w_query, w_key, w_value, w_out, w_gate, w_up, w_down, norm_attn, norm_mlp):
        n_tok, width = tokens.shape[1], tokens.shape[2]
        ffn = w_gate.shape[1]
        rows, sub = n_tok // N_ROWCH, n_tok // N_ROWCH // N_REL
        q_cols, kv_cols = w_query.shape[1], w_key.shape[1]
        c_cols = width // N_DOWN
        n_units = 2 * N_DOWN
        freqs = jnp.tile(rope_freqs(), 2)[None]
        vm = pl.BlockSpec(memory_space=pltpu.VMEM)
        smem = pl.BlockSpec(memory_space=pltpu.SMEM)
        hbm = pl.BlockSpec(memory_space=pl.ANY)
        n_groups = 4 + len(GU_SPLIT) - 1 + N_DOWN
        n_y = N_ROWCH + n_units
        st = lambda *s: jax.ShapeDtypeStruct(s, BF16)
        dma = pltpu.SemaphoreType.DMA
        outs = pl.pallas_call(
            functools.partial(layer_kernel, n_tp, n_fsdp),
            out_shape=[st(n_tok, 2 * kv_cols), st(n_units, N_REL, sub, 2 * c_cols),
                       st(width, 2 * kv_cols + q_cols), st(w_out.shape[0], width),
                       st(width, ffn), st(width, ffn), st(N_DOWN, ffn, c_cols), st(n_tok, ffn), st(n_y, 3, sub, width)],
            in_specs=[smem] * 2 + [vm] * 3 + [hbm] * 8,
            out_specs=[hbm] * 9,
            scratch_shapes=[
                pltpu.VMEM((n_tok, width), BF16), pltpu.VMEM((2, width, 2 * TILE), BF16),
                pltpu.VMEM((2, rows, width), BF16),
                pltpu.VMEM((rows, width), BF16), pltpu.VMEM((n_tok, 2 * kv_cols + q_cols), BF16),
                pltpu.VMEM((2, rows, q_cols), BF16), pltpu.VMEM((3, sub, width), BF16),
                pltpu.VMEM((2, sub, 2 * c_cols), BF16), pltpu.VMEM((2, 2 * rows, TILE), BF16),
                pltpu.VMEM((n_tok, HEAD_DIM), F32), pltpu.VMEM((n_tok, HEAD_DIM), F32), pltpu.VMEM((1, n_tok), F32),
                pltpu.VMEM((2, width), F32),
                dma((n_groups,)), dma((n_groups, 4)), dma((n_y, 3)), dma((n_y, 4)),
                dma((4,)), dma((4,)), dma((5,)), dma((2, 11)), dma((2,)), dma((5,)), dma((n_fsdp,)),
            ],
            compiler_params=pltpu.CompilerParams(vmem_limit_bytes=67043328, collective_id=0, has_side_effects=True),
            name="layer",
        )(positions, valid_len, freqs, norm_attn, norm_mlp, tokens[0],
          w_key, w_value, w_query, w_out, w_gate, w_up, w_down)
        kv_all, res = outs[0], outs[1]
        hidden, key_cache, value_cache = place(res, kv_all, n_tok, width, n_tp, n_fsdp)
        return hidden[None], key_cache[None], value_cache[None]

    return jax.shard_map(local_layer, mesh=mesh, in_specs=in_specs, out_specs=out_specs, check_vma=False)
```

```python
import functools
import math
import jax
import jax.numpy as jnp
from jax import lax
from jax.experimental import pallas as pl
from jax.experimental.pallas import tpu as pltpu
from jax.sharding import PartitionSpec as P

HEAD_DIM = 128
ROPE_THETA = 500000.0
NORM_EPS = 1e-5
SCORE_SCALE = HEAD_DIM ** -0.5
LOG2E = 1.4426950408889634
BF16 = jnp.bfloat16
F32 = jnp.float32
N_REL = 4
HALVES = (0, 1)
N_ROWCH = 4
N_DOWN = 4
TILE = 256
GU_SPLIT = (0, 2, 6, 10, 14)
MESH = pl.DeviceIdType.MESH
VMEM_PLACE = 67043328


def rope_freqs():
    half_idx = jnp.arange(HEAD_DIM // 2, dtype=F32)
    inv_freq = jnp.power(ROPE_THETA, -2.0 * half_idx / HEAD_DIM)
    wave_len = 2.0 * math.pi / inv_freq
    smooth = (8192.0 / wave_len - 1.0) / 3.0
    blended = (1.0 - smooth) * inv_freq / 8.0 + smooth * inv_freq
    return jnp.where(wave_len < 2048.0, inv_freq, jnp.where(wave_len > 8192.0, inv_freq / 8.0, blended))


def upto(n):
    return pl.ds(0, n)


def layer_kernel(n_tp, n_fsdp, *refs):
    (pos_ref, len_ref, freq_ref, gain_a, gain_m, tok, wk, wv, wq, wo, wg, wu, wd,
     kv_out, res, full_p, full_o, full_g, full_u, full_d, act, rs,
     u_buf, w_buf, p_buf, x1_buf, qkv_buf, o_buf, stage, r_buf, a_stage, cos_ref, sin_ref, bias_ref, gains,
     x_send, x_recv, y_send, y_recv, w_sem, wd_sem, l_sem, b_sem, a_sem, r_sem, o_sem) = refs
    n_tok, width = tok.shape
    rows = n_tok // N_ROWCH
    sub = rows // N_REL
    k_rows = wk.shape[0]
    kv_cols = wk.shape[1]
    q_cols = wq.shape[1]
    ffn = wg.shape[1]
    o_cols = wo.shape[1]
    d_cols = wd.shape[1] // N_DOWN
    c_cols = d_cols * n_fsdp
    n_x = n_fsdp // 2

    me_t = lax.axis_index("tp")
    me_f = lax.axis_index("fsdp")
    chip, core = me_f // 2, me_f % 2
    t_right = lax.rem(me_t + 1, n_tp)
    t_left = lax.rem(me_t + n_tp - 1, n_tp)
    f_right = 2 * lax.rem(chip + 1, n_x) + core
    f_left = 2 * lax.rem(chip + n_x - 1, n_x) + core
    f_far = 2 * lax.rem(chip + 2, n_x) + core
    other = 1 - 2 * core
    f_twin = me_f + other

    barrier = pltpu.get_barrier_semaphore()
    for peer in ({"tp": t_left}, {"tp": t_right}, {"fsdp": f_left}, {"fsdp": f_right}, {"fsdp": f_twin}):
        pl.semaphore_signal(barrier, inc=1, device_id=peer, device_id_type=MESH)
    pl.semaphore_wait(barrier, 5)

    def al(val, mult):
        return pl.multiple_of(val, mult)

    groups = []

    def add_group(pieces, area):
        groups.append((pieces, area))
        return len(groups) - 1

    def by_rows(full, c0, n):
        return lambda f: full.at[pl.ds(al(f * k_rows, k_rows), k_rows), pl.ds(c0, n)]

    def halves(own, place):
        n = own.shape[0] // 2
        return [(own.at[pl.ds(i * n, n), :], lambda f, i=i: place(f).at[pl.ds(i * n, n), :], i) for i in HALVES]

    def o_piece(f):
        return full_o.at[:, pl.ds(al(f * o_cols, o_cols), o_cols)]

    def d_piece(k, f):
        return full_d.at[k, :, pl.ds(al(f * d_cols, d_cols), d_cols)]

    half_q = q_cols // 2
    q_from = 2 * kv_cols

    def row_area(full, c0, cols):
        return lambda n: full.at[upto(n * k_rows), pl.ds(c0, cols)]

    pkv = add_group([(own, by_rows(full_p, i * kv_cols, kv_cols), i) for i, own in enumerate((wk, wv))], row_area(full_p, 0, q_from))
    q0, q1 = [add_group([(wq.at[:, pl.ds(i * half_q, half_q)], by_rows(full_p, q_from + i * half_q, half_q), i)],
                        row_area(full_p, q_from + i * half_q, half_q)) for i in HALVES]
    po = add_group(halves(wo, o_piece), lambda n: full_o.at[:, upto(n * o_cols)])
    g0, g1, g2, g3 = [
        add_group([(own.at[:, pl.ds(lo * TILE, (hi - lo) * TILE)], by_rows(full, lo * TILE, (hi - lo) * TILE), i)
                   for i, (own, full) in enumerate(((wg, full_g), (wu, full_u)))], row_area(full_g, 0, 2 * (hi - lo) * TILE))
        for lo, hi in zip(GU_SPLIT, GU_SPLIT[1:])]
    d0, d1, d2, d3 = [
        add_group(halves(wd.at[:, pl.ds(k * d_cols, d_cols)], functools.partial(d_piece, k)), lambda n, k=k: full_d.at[k, :, upto(n * d_cols)])
        for k in range(N_DOWN)]

    FIRST, FAR_ON, TWIN = HALVES, 2, 3

    def x_copy(g, i, m):
        own, place, way = groups[g][0][i]
        near = (f_left, f_right)
        if m in FIRST:
            src, owner, target = own, me_f, near[1 - m]
        elif m == FAR_ON:
            owner, target = near[way], near[1 - way]
            src = place(owner)
        else:
            owner, target = (me_f, f_left, f_right, f_far)[m - TWIN], f_twin
            src = own if m == TWIN else place(owner)
        return pltpu.make_async_remote_copy(src_ref=src, dst_ref=place(owner), send_sem=x_send.at[g], recv_sem=x_recv.at[g, min(m, TWIN)],
                                            device_id={"fsdp": target}, device_id_type=MESH)

    def x_all(g, *ms):
        for m in ms:
            for i in range(len(groups[g][0])):
                x_copy(g, i, m).start()

    def x_taken(g, kind, n=1):
        area = groups[g][1](n)
        return pltpu.make_async_remote_copy(src_ref=area, dst_ref=area, send_sem=x_send.at[g], recv_sem=x_recv.at[g, kind],
                                            device_id={"fsdp": f_twin}, device_id_type=MESH)

    def x_first(*gs):
        for g in gs:
            x_all(g, *FIRST, TWIN)

    def x_fwd(g):
        for i, piece in enumerate(groups[g][0]):
            x_taken(g, piece[2]).wait_recv()
            x_copy(g, i, FAR_ON).start()

    def x_side(g):
        if len(groups[g][0]) == 1:
            x_taken(g, 1 - groups[g][0][0][2]).wait_recv()
        x_all(g, TWIN + 1, TWIN + 2)

    def x_second(g):
        x_fwd(g)
        x_side(g)

    def x_third(g):
        x_taken(g, FAR_ON).wait_recv()
        x_all(g, TWIN + 3)

    def x_ready(g):
        x_taken(g, TWIN, 4).wait_recv()

    def x_sent(*gs):
        for g in gs:
            x_taken(g, TWIN, 7).wait_send()

    unit_list = [(k, pair) for pair in range(2) for k in range(N_DOWN)]
    unit_at = [2 * k + pair for k, pair in unit_list]
    unit_order = {u: i for i, u in enumerate(unit_at)}

    def y_rows(e):
        if e < N_ROWCH:
            slot, lane, wid = e % 2, 0, width
        else:
            q = unit_order[e - N_ROWCH] % 4
            slot, lane, wid = q // 2, (q % 2) * (width // 2), 2 * c_cols
        return slot, lane, wid

    def lanes(e, h):
        slot, lane, wid = y_rows(e)
        return slot, pl.ds(lane + h * (wid // 2), wid // 2), pl.ds(h * (wid // 2), wid // 2)

    def g_slice(e, r):
        if e < N_ROWCH:
            return u_buf.at[pl.ds(e * rows + r * sub, sub), :]
        return res.at[e - N_ROWCH, r]

    FAR, NEAR, SUM, RIGHT, LEFT, PASS = range(6)
    OUT, SPREAD, ON = range(3)
    sent_as = (OUT, OUT, OUT, SPREAD, SPREAD, ON)
    GOT_FAR, GOT_SUMS, GOT_SPREAD, GOT_REST = range(4)

    def got_as(e, m, h):
        if m in (RIGHT, LEFT):
            return GOT_SPREAD if e < N_ROWCH or m == LEFT - h else GOT_REST
        return {FAR: GOT_FAR, PASS: GOT_REST}.get(m, GOT_SUMS)

    def y_taken(e, kind, n):
        area = rs.at[e, upto(n), :, upto(y_rows(e)[2])]
        return pltpu.make_async_remote_copy(src_ref=area, dst_ref=area, send_sem=y_send.at[e, min(kind, ON)], recv_sem=y_recv.at[e, kind],
                                            device_id={"tp": t_right}, device_id_type=MESH)

    def y_copy(e, m, h=0):
        slot, here, there = lanes(e, h)
        if m in (RIGHT, LEFT):
            src, dst, to = g_slice(e, 0), g_slice(e, m - 2), m - 3
            if e >= N_ROWCH:
                src, dst = r_buf.at[unit_order[e - N_ROWCH] % 2, :, there], dst.at[:, there]
        elif m == PASS:
            src, dst, to = g_slice(e, 2 - h).at[:, there], g_slice(e, 3).at[:, there], 1 - h
        else:
            r, i, to = {FAR: (3, 0, h), NEAR: (1 + h, 2 - h, 1 - h), SUM: (2 - h, 1 + h, h)}[m]
            src, dst = p_buf.at[slot, pl.ds(r * sub, sub), here], rs.at[e, i, :, there]
        return pltpu.make_async_remote_copy(src_ref=src, dst_ref=dst, send_sem=y_send.at[e, sent_as[m]], recv_sem=y_recv.at[e, got_as(e, m, h)],
                                            device_id={"tp": t_right if to == 0 else t_left}, device_id_type=MESH)

    def rs_slice(e, i):
        return rs.at[e, i, :, upto(y_rows(e)[2])]

    def load_stage(e, idx):
        wid = y_rows(e)[2]
        for i in idx:
            pltpu.make_async_copy(rs_slice(e, i), stage.at[i, :, upto(wid)], l_sem.at[i]).start()

    def wait_stage(e, idx):
        wid = y_rows(e)[2]
        for i in idx:
            pltpu.make_async_copy(rs_slice(e, i), stage.at[i, :, upto(wid)], l_sem.at[i]).wait()

    def y_start(e, hs=HALVES):
        for m in (FAR, NEAR):
            for h in hs:
                y_copy(e, m, h).start()

    def y_have(e):
        y_taken(e, GOT_SUMS, 2).wait_recv()

    def y_send_all(e):
        y_copy(e, LEFT).start()
        y_copy(e, RIGHT).start()

    def y_sent_all(e):
        y_taken(e, SPREAD, 2).wait_send()

    EW = 32

    def y_add(e):
        y_taken(e, GOT_FAR, 1).wait_recv()
        for h in HALVES:
            there = lanes(e, h)[2]
            pltpu.make_async_copy(rs.at[e, 0, :, there], stage.at[0, :, there], l_sem.at[h]).start()
        for h in HALVES:
            slot, here, there = lanes(e, h)
            pltpu.make_async_copy(rs.at[e, 0, :, there], stage.at[0, :, there], l_sem.at[h]).wait()

            def body(i, carry, h=h, here=here, there=there):
                rr = pl.ds(al((2 - h) * sub + i * EW, EW), EW)
                tot = p_buf[slot, rr, here].astype(F32) + stage[0, pl.ds(al(i * EW, EW), EW), there].astype(F32)
                p_buf[slot, rr, here] = tot.astype(BF16)
                return carry

            lax.fori_loop(0, sub // EW, body, 0)
            y_copy(e, SUM, h).start()

    def tok_copy(c):
        row0 = al(c * rows + me_t * sub, sub)
        return pltpu.make_async_copy(tok.at[pl.ds(row0, sub), :], stage.at[0], l_sem.at[3])

    def y_norm(c):
        slot = c % 2
        tok_copy(c).start()
        y_have(c)
        load_stage(c, (1, 2))
        wait_stage(c, (1, 2))
        tok_copy(c).wait()

        def body(i, carry):
            rr = al(i * EW, EW)
            here = pl.ds(rr, EW)
            tot = p_buf[slot, here, :].astype(F32) + stage[1, here, :].astype(F32) + stage[2, here, :].astype(F32)
            x1 = (stage[0, here, :].astype(F32) + tot).astype(BF16)
            x1_buf[pl.ds(al(c * sub + i * EW, EW), EW), :] = x1
            xf = x1.astype(F32)
            inv = lax.rsqrt(jnp.mean(xf * xf, axis=-1, keepdims=True) + NORM_EPS)
            u_buf[pl.ds(al(c * rows + i * EW, EW), EW), :] = (xf * inv * gains[1:, :]).astype(BF16)
            return carry

        lax.fori_loop(0, sub // EW, body, 0)
        y_send_all(c)

    def y_final(k, pair):
        unit = 2 * k + pair
        e = N_ROWCH + unit
        r_slot = unit_order[unit] % 2
        if unit_order[unit] >= 2:
            before = N_ROWCH + unit_at[unit_order[unit] - 2]
            y_sent_all(before)
            r_out(before).wait()
        y_have(e)
        loads = [[pltpu.make_async_copy(rs.at[e, i, :, lanes(e, h)[2]], stage.at[i, :, lanes(e, h)[2]], l_sem.at[2 * h + i - 1])
                  for i in (1, 2)] for h in HALVES]
        for cp in loads[0] + loads[1]:
            cp.start()
        for h in HALVES:
            slot, mine, there = lanes(e, h)
            for cp in loads[h]:
                cp.wait()

            def body(i, carry, h=h, slot=slot, mine=mine):
                here = pl.ds(al(i * EW, EW), EW)
                x_rows = pl.ds(al((2 * pair + h) * sub + i * EW, EW), EW)
                for f in range(n_fsdp):
                    at = pl.ds(h * c_cols + f * d_cols, d_cols)
                    tot = (p_buf[slot, here, pl.ds(mine.start + f * d_cols, d_cols)].astype(F32)
                           + stage[1, here, at].astype(F32) + stage[2, here, at].astype(F32))
                    x1 = x1_buf[x_rows, pl.ds((f * N_DOWN + k) * d_cols, d_cols)].astype(F32)
                    r_buf[r_slot, here, at] = (x1 + tot).astype(BF16)
                return carry

            lax.fori_loop(0, sub // EW, body, 0)
        for m, h in ((LEFT, 0), (RIGHT, 1), (LEFT, 1), (RIGHT, 0)):
            y_copy(e, m, h).start()
        r_out(e).start()

    def r_out(e):
        return pltpu.make_async_copy(r_buf.at[unit_order[e - N_ROWCH] % 2], res.at[e - N_ROWCH, 0], r_sem.at[unit_order[e - N_ROWCH] % 2])

    def y_pass(e):
        y_taken(e, GOT_SPREAD, 2 if e < N_ROWCH else 1).wait_recv()
        for h in HALVES:
            y_copy(e, PASS, h).start()

    def y_ready(e):
        y_taken(e, GOT_REST, 1 if e < N_ROWCH else 2).wait_recv()

    def bounce(src, via, dst, i):
        return pltpu.make_async_copy(src, via, b_sem.at[0, i]), pltpu.make_async_copy(via, dst, b_sem.at[1, i])

    small = [
        bounce(wk, w_buf.at[0, upto(k_rows), upto(kv_cols)], by_rows(full_p, 0, kv_cols)(me_f), 0),
        bounce(wv, w_buf.at[0, upto(k_rows), pl.ds(kv_cols, kv_cols)], by_rows(full_p, kv_cols, kv_cols)(me_f), 1),
        bounce(wq.at[:, upto(half_q)], w_buf.at[0, pl.ds(k_rows, k_rows), :], by_rows(full_p, q_from, half_q)(me_f), 2),
        bounce(wq.at[:, pl.ds(half_q, half_q)], w_buf.at[0, pl.ds(2 * k_rows, k_rows), :], by_rows(full_p, q_from + half_q, half_q)(me_f), 3),
        bounce(wo, w_buf.at[0, pl.ds(3 * k_rows, wo.shape[0]), :], o_piece(me_f), 4),
    ] + [
        bounce(wd.at[:, pl.ds(k * d_cols, d_cols)], w_buf.at[1, upto(ffn), pl.ds(k * d_cols, d_cols)], d_piece(k, me_f), 5 + k)
        for k in range(N_DOWN)
    ]
    large = [
        bounce(wg, p_buf.at[0, :, upto(ffn)], by_rows(full_g, 0, ffn)(me_f), 9),
        bounce(wu, p_buf.at[1, :, upto(ffn)], by_rows(full_u, 0, ffn)(me_f), 10),
    ]

    def bounce_in(group):
        for a, _ in group:
            a.start()

    def bounce_out(group):
        for a, b in group:
            a.wait()
            b.start()

    def bounce_end(group):
        for _, b in group:
            b.wait()

    def norm_rows(late):
        n_tile = n_tok // rows

        def load(i):
            return pltpu.make_async_copy(tok.at[pl.ds(i * rows, rows), :], p_buf.at[i % 2], w_sem.at[i % 2])

        load(0).start()
        for i in range(n_tile):
            if i + 1 < n_tile:
                load(i + 1).start()
            load(i).wait()

            def body(j, carry, i=i):
                vals = p_buf[i % 2, pl.ds(al(j * EW, EW), EW), :].astype(F32)
                inv = lax.rsqrt(jnp.mean(vals * vals, axis=-1, keepdims=True) + NORM_EPS)
                u_buf[pl.ds(al(i * rows + j * EW, EW), EW), :] = (vals * inv * gains[:1, :]).astype(BF16)
                return carry

            lax.fori_loop(0, rows // EW, body, 0)
            if i == n_tile - 2:
                late()

    def tables():
        sign = jnp.where(lax.broadcasted_iota(jnp.int32, (1, HEAD_DIM), 1) < HEAD_DIM // 2, -1.0, 1.0)
        first = pos_ref[0, 0]

        def body(i, carry):
            here = pl.ds(al(i * sub, sub), sub)
            row = first + i * sub + lax.broadcasted_iota(jnp.int32, (sub, HEAD_DIM), 0)
            angle = row.astype(F32) * freq_ref[...]
            cos_ref[here, :] = jnp.cos(angle)
            sin_ref[here, :] = sign * jnp.sin(angle)
            return carry

        lax.fori_loop(0, n_tok // sub, body, 0)
        key = lax.broadcasted_iota(jnp.int32, (1, n_tok), 1)
        bias_ref[...] = jnp.where(key < len_ref[0], 0.0, -jnp.inf)

    def stream(n0, n1, load, compute, hooks={}, lazy=(), fetched=False, then=None):
        def fetch(n, slot):
            for cp in load(n, slot):
                cp.start()

        if not fetched:
            fetch(n0, 0)

        def body(n, carry):
            slot = lax.rem(n - n0, 2)
            late = functools.reduce(jnp.logical_or, [n + 1 == at for at in lazy], n + 1 >= n1)
            pl.when(jnp.logical_not(late))(lambda: fetch(n + 1, 1 - slot))
            if then:
                pl.when(n + 1 == n1)(then)
            for cp in load(n, slot):
                cp.wait()
            compute(n, slot)
            for at, todo in hooks.items():
                @pl.when(n == at)
                def _(at=at, todo=todo):
                    todo()
                    if at + 1 in lazy:
                        fetch(at + 1, 1 - slot)
            return carry

        lax.fori_loop(n0, n1, body, 0)

    def project(hooks, lazy):
        def load(n, slot):
            return (pltpu.make_async_copy(full_p.at[:, pl.ds(al(n * TILE, TILE), TILE)], w_buf.at[slot, :, upto(TILE)], w_sem.at[slot]),)

        def compute(n, slot):
            plain = n == 1

            def body(m, carry):
                here = pl.ds(al(m * 2 * rows, rows), 2 * rows)
                acc = jnp.dot(u_buf[here, :], w_buf[slot, :, :TILE], preferred_element_type=F32)
                cos_t = jnp.where(plain, 1.0, cos_ref[here, :])
                sin_t = jnp.where(plain, 0.0, sin_ref[here, :])
                for h in range(TILE // HEAD_DIM):
                    val = acc[:, h * HEAD_DIM:(h + 1) * HEAD_DIM]
                    val = val * cos_t + pltpu.roll(val, HEAD_DIM // 2, 1) * sin_t
                    qkv_buf[here, pl.ds(al(n * TILE + h * HEAD_DIM, HEAD_DIM), HEAD_DIM)] = val.astype(BF16)
                return carry

            lax.fori_loop(0, n_tok // (2 * rows), body, 0)

        stream(0, full_p.shape[1] // TILE, load, compute, hooks, lazy)

    def attend(c, mid=None):
        blk = 2 * sub
        n_blk = rows // blk
        n_old = c * rows
        n_head = q_cols // HEAD_DIM
        per_grp = q_cols // kv_cols
        dims = (((1,), (1,)), ((), ()))
        here = pl.ds(n_old, rows)

        def body(idx, carry):
            head = idx // n_blk
            part = lax.rem(idx, n_blk)
            row0 = al(part * blk, blk)
            col0 = al(head * HEAD_DIM, HEAD_DIM)
            k_at = al((head // per_grp) * HEAD_DIM, HEAD_DIM)
            k_cols, v_cols = pl.ds(k_at, HEAD_DIM), pl.ds(al(kv_cols + k_at, HEAD_DIM), HEAD_DIM)
            q_blk = qkv_buf[pl.ds(al(n_old + row0, blk), blk), pl.ds(al(q_from + col0, HEAD_DIM), HEAD_DIM)]
            s_new = lax.dot_general(q_blk, qkv_buf[here, k_cols], dims, preferred_element_type=F32)
            s_new = s_new * (SCORE_SCALE * LOG2E) + bias_ref[:, here]
            q_idx = row0 + lax.broadcasted_iota(jnp.int32, (blk, rows), 0)
            k_idx = lax.broadcasted_iota(jnp.int32, (blk, rows), 1)
            s_new = jnp.where(k_idx <= q_idx, s_new, -jnp.inf)
            top = jnp.max(s_new, axis=1, keepdims=True)
            if n_old:
                s_old = lax.dot_general(q_blk, qkv_buf[:n_old, k_cols], dims, preferred_element_type=F32)
                s_old = s_old * (SCORE_SCALE * LOG2E) + bias_ref[:, :n_old]
                top = jnp.maximum(top, jnp.max(s_old, axis=1, keepdims=True))
            p_new = jnp.exp2(s_new - top)
            den = jnp.sum(p_new, axis=1, keepdims=True)
            acc = jnp.dot(p_new.astype(BF16), qkv_buf[here, v_cols], preferred_element_type=F32)
            if n_old:
                p_old = jnp.exp2(s_old - top)
                den = den + jnp.sum(p_old, axis=1, keepdims=True)
                acc = acc + jnp.dot(p_old.astype(BF16), qkv_buf[:n_old, v_cols], preferred_element_type=F32)
            out = (acc / den).astype(BF16)
            for s in range(blk // sub):
                dist = lax.rem(part * (blk // sub) + s - me_t + n_tp, n_tp)
                pos = jnp.where(dist == 0, 0, jnp.where(dist == n_tp - 1, 1, dist + 1))
                o_buf[c % 2, pl.ds(al(pos * sub, sub), sub), pl.ds(col0, HEAD_DIM)] = out[s * sub:(s + 1) * sub, :]
            if mid:
                pl.when(idx == n_head)(mid)
            return carry

        lax.fori_loop(0, n_head * n_blk, body, 0)

    def o_place(n):
        depth = wo.shape[0]
        per = width // depth
        return n // per, pl.ds(al(lax.rem(n, per) * depth, depth), depth)

    def o_tile(n):
        slot, here = o_place(n)
        return pltpu.make_async_copy(full_o.at[:, pl.ds(al(n * o_cols, o_cols), o_cols)], w_buf.at[slot, here, :], o_sem.at[n])

    def out_load():
        def body(n, carry):
            o_tile(n).start()
            return carry

        lax.fori_loop(0, n_fsdp, body, 0)

    def out_project(c):
        def body(n, carry):
            if c == 0:
                o_tile(n).wait()
            slot, here = o_place(n)
            acc = jnp.dot(o_buf[c % 2], w_buf[slot, here, :], preferred_element_type=F32)
            p_buf[c % 2, :, pl.ds(al(n * o_cols, o_cols), o_cols)] = acc.astype(BF16)
            return carry

        lax.fori_loop(0, n_fsdp, body, 0)

    def act_copy(c0, nc, n, slot):
        return pltpu.make_async_copy(a_stage.at[slot, upto(nc * rows), :],
                                     act.at[pl.ds(c0 * rows, nc * rows), pl.ds(al(n * TILE, TILE), TILE)], a_sem.at[slot])

    def gate_up(pair, n0, n1, hooks={}):
        c0, nc = 2 * pair, 2
        def load(n, slot):
            here = pl.ds(al(n * TILE, TILE), TILE)
            return (pltpu.make_async_copy(full_g.at[:, here], w_buf.at[slot, :, upto(TILE)], w_sem.at[slot]),
                    pltpu.make_async_copy(full_u.at[:, here], w_buf.at[slot, :, pl.ds(TILE, TILE)], w_sem.at[2 + slot]))

        def compute(n, slot):
            lhs = u_buf[c0 * rows:(c0 + nc) * rows, :]
            gate = jnp.dot(lhs, w_buf[slot, :, :TILE], preferred_element_type=F32)
            gate = gate * jax.nn.sigmoid(gate)
            val = gate * jnp.dot(lhs, w_buf[slot, :, TILE:], preferred_element_type=F32)

            @pl.when(n - n0 >= 2)
            def _():
                act_copy(c0, nc, n, slot).wait()
            a_stage[slot, :nc * rows, :] = val.astype(BF16)
            act_copy(c0, nc, n, slot).start()

        stream(n0, n1, load, compute, hooks)
        for i in range(min(2, n1 - n0)):
            act_copy(c0, nc, n1 - 1, (n1 - 1 - i - n0) % 2).wait()

    def load_act(c):
        here = pl.ds(c * rows, rows)
        return pltpu.make_async_copy(act.at[here, :], u_buf.at[here, upto(ffn)], r_sem.at[3 + c % 2])

    def down_place(slot, i):
        return upto(ffn // 2), pl.ds(al((2 * slot + i) * TILE, TILE), TILE)

    def down_tile(k, n, slot):
        return [pltpu.make_async_copy(full_d.at[k, pl.ds(i * (ffn // 2), ffn // 2), pl.ds(al(n * TILE, TILE), TILE)],
                                      qkv_buf.at[down_place(slot, i)], wd_sem.at[2 * slot + i]) for i in HALVES]

    def down_fetch(k):
        for cp in down_tile(k, 0, 0):
            cp.start()

    def down(k, pair, cs, fetched, then):
        e = N_ROWCH + 2 * k + pair
        slot_p, lane, _ = y_rows(e)
        half = ffn // 2
        row0, n_row = (2 * pair + cs[0]) * rows, len(cs) * rows

        def compute(n, slot):
            prod = sum(jnp.dot(u_buf[row0:row0 + n_row, i * half:(i + 1) * half], qkv_buf[down_place(slot, i)], preferred_element_type=F32)
                       for i in HALVES).astype(BF16)
            for i, ci in enumerate(cs):
                p_buf[slot_p, :, pl.ds(al(lane + ci * c_cols + n * TILE, TILE), TILE)] = prod[i * rows:(i + 1) * rows, :]

        stream(0, c_cols // TILE, functools.partial(down_tile, k), compute, fetched=fetched, then=then)

    def sent(e):
        y_taken(e, OUT, 3).wait_send()

    def passed(e):
        y_taken(e, ON, 1).wait_send()

    def scoped(fn):
        def run(*args, **kw):
            with jax.named_scope("_".join([fn.__name__] + [str(a) for a in args if isinstance(a, int)])):
                return fn(*args, **kw)
        return run

    x_first, x_fwd, x_side, x_third, x_ready = map(scoped, (x_first, x_fwd, x_side, x_third, x_ready))
    y_start, y_add, y_norm, y_final, y_pass, y_ready = map(scoped, (y_start, y_add, y_norm, y_final, y_pass, y_ready))
    norm_rows, project, attend, out_project, gate_up, down = map(scoped, (norm_rows, project, attend, out_project, gate_up, down))
    tables, bounce_in, bounce_out, bounce_end, sent = map(scoped, (tables, bounce_in, bounce_out, bounce_end, sent))

    def x_done(g):
        x_third(g)
        x_ready(g)

    def sent_u(*cs):
        for c in cs:
            y_sent_all(c)
            passed(c)

    c0, c1, c2, c3 = range(N_ROWCH)
    units = [N_ROWCH + u for u in unit_at]
    t0, t1, t2, t3, t4 = GU_SPLIT

    def begin(i, fetched=False, ahead=False, wait=None):
        if i >= 4:
            sent(units[i - 4])
        k, pair = unit_list[i]
        parts = [(h,) for h in HALVES] if wait else (HALVES,)
        for cs in parts:
            last = cs == parts[-1]
            then = functools.partial(down_fetch, unit_list[i + 1][0]) if last and ahead else None if last else functools.partial(down_fetch, k)
            if wait:
                wait(cs[0])
            down(k, pair, cs, fetched or cs != parts[0], then)
            y_start(units[i], cs)

    x_first(pkv, q0)
    bounce_in(small)
    gains[:1, :] = gain_a[...].astype(F32)[None]
    gains[1:, :] = gain_m[...].astype(F32)[None]
    norm_rows(lambda: x_second(pkv))
    bounce_out(small)
    bounce_in(large)
    tables()
    x_fwd(q0)
    x_first(q1)
    x_done(pkv)
    bounce_end(small)
    kv_copy = pltpu.make_async_copy(qkv_buf.at[:, upto(q_from)], kv_out, r_sem.at[2])

    def have_kv():
        bounce_out(large)
        kv_copy.start()
        x_side(q0)
        x_done(q0)

    project({
        0: lambda: (x_fwd(q1), x_first(po)),
        1: have_kv,
        3: lambda: (x_side(q1), x_done(q1)),
        4: lambda: (x_second(po), x_first(g0, g1, g2)),
    }, (2, 4))
    attend(c0)
    x_done(po)
    out_load()
    bounce_end(large)
    out_project(c0)
    y_start(c0)
    attend(c1)
    out_project(c1)
    y_start(c1)
    x_second(g0)
    attend(c2, lambda: y_add(c0))
    attend(c3, lambda: y_add(c1))
    x_second(g1)
    y_norm(c0)
    y_norm(c1)
    sent(c0)
    out_project(c2)
    sent(c1)
    out_project(c3)
    y_pass(c0)
    y_pass(c1)
    y_start(c2)
    y_start(c3)
    x_second(g2)
    x_first(g3)
    x_third(g0)
    x_third(g1)
    x_ready(g0)
    y_ready(c0)
    y_ready(c1)
    x_ready(g1)
    gate_up(0, t0, t3, {t1: lambda: (x_third(g2), y_add(c2)), t2 - 2: lambda: x_ready(g2), t2 + 1: lambda: y_add(c3)})
    x_second(g3)
    x_first(d0)
    y_norm(c2)
    y_norm(c3)
    x_done(g3)
    y_pass(c2)
    gate_up(0, t3, t4, {t3 + 1: lambda: (x_second(d0), x_first(d1)), t4 - 2: lambda: y_pass(c3)})
    sent_u(c0, c1)
    load_act(c0).start()
    load_act(c1).start()
    kv_copy.wait()
    x_done(d0)
    down_fetch(0)
    sent(c2)
    sent(c3)
    (load_act(c0).wait(), load_act(c1).wait(), begin(0, True))
    x_second(d1)
    x_first(d2)
    y_ready(c2)
    y_ready(c3)
    sent_u(c2, c3)
    f0, f1, f2, f3 = units[:N_DOWN]
    gate_up(1, t0, t4, {
        1: lambda: (y_add(f0), x_done(d1), begin(1)),
        2: lambda: y_final(*unit_list[0]),
        3: lambda: (x_second(d2), x_first(d3)),
        4: lambda: y_add(f1),
        5: lambda: x_third(d2),
        6: lambda: (y_pass(f0), y_final(*unit_list[1]), x_ready(d2), begin(2), x_second(d3)),
        8: lambda: y_pass(f1),
        9: lambda: (y_add(f2), x_done(d3), begin(3)),
        10: lambda: y_final(*unit_list[2]),
        12: lambda: (y_add(f3), down_fetch(0)),
    })
    load_act(c2).start()
    load_act(c3).start()
    y_pass(f2)
    n_unit = len(units)
    half = n_unit // 2
    begin(half, True, True, lambda h: load_act(2 + h).wait())
    y_final(*unit_list[half - 1])
    for i in range(half, n_unit):
        if i + 1 < n_unit:
            begin(i + 1, True, i + 2 < n_unit)
        if i == half:
            y_add(units[i])
        x_sent(*range(len(groups) * (i - half) // half, len(groups) * (i + 1 - half) // half))
        y_pass(units[i - 1])
        if i > half:
            y_ready(units[i - 2])
            passed(units[i - 2])
        if i + 1 < n_unit:
            y_add(units[i + 1])
        y_final(*unit_list[i])
    for e in units[-4:]:
        sent(e)
    y_pass(units[-1])
    for e in units[:half - 1] + units[-2:]:
        y_ready(e)
        passed(e)
    for e in units[-2:]:
        y_sent_all(e)
        r_out(e).wait()


def place_kernel(n_tp, n_fsdp, res, kv, out, key_out, value_out, in_buf, out_buf, kv_buf, cache_buf, in_sem, out_sem, kv_sem, cache_sem):
    sub, c_cols = res.shape[2], res.shape[3] // 2
    cols = c_cols // n_fsdp
    me_t = lax.axis_index("tp")

    def load(c, k):
        src = res.at[2 * k + c // 2, :, :, pl.ds(pl.multiple_of(lax.rem(c, 2) * c_cols, c_cols), c_cols)]
        return pltpu.make_async_copy(src, in_buf.at[c, k], in_sem.at[c])

    def store(c, r):
        here = pl.ds(pl.multiple_of((c * N_REL + r) * sub, sub), sub)
        return pltpu.make_async_copy(out_buf.at[here, :], out.at[here, :], out_sem.at[c, r])

    def caches():
        return [pltpu.make_async_copy(cache_buf.at[i], dst, cache_sem.at[i]) for i, dst in enumerate((key_out, value_out))]

    for c in range(N_ROWCH):
        for k in range(N_DOWN):
            load(c, k).start()
    kv_load = pltpu.make_async_copy(kv, kv_buf, kv_sem)
    kv_load.start()

    def chunk(c, carry):
        pltpu.make_async_copy(res.at[upto(N_DOWN), :, :, upto(c_cols)], in_buf.at[c], in_sem.at[c]).wait()
        for r, dist in enumerate((0, n_tp - 1, 1, 2)):
            row = lax.rem(me_t + dist, n_tp)
            here = pl.ds(pl.multiple_of((c * N_REL + row) * sub, sub), sub)
            for k in range(N_DOWN):
                for f in range(n_fsdp):
                    c0 = (f * N_DOWN + k) * cols
                    out_buf[here, c0:c0 + cols] = in_buf[c, k, r, :, f * cols:(f + 1) * cols]
            store(c, row).start()
        return carry

    lax.fori_loop(0, N_ROWCH, chunk, 0)
    kv_load.wait()
    for i in HALVES:
        n = kv.shape[1] // 2
        cache_buf[i] = kv_buf[:, i * n:(i + 1) * n].reshape(cache_buf.shape[1:])
    for cp in caches():
        cp.start()

    def finish(c, carry):
        for r in range(N_REL):
            store(c, r).wait()
        return carry

    lax.fori_loop(0, N_ROWCH, finish, 0)
    for cp in caches():
        cp.wait()


def place(res, kv_all, n_tok, width, n_tp, n_fsdp):
    sub, c_cols = res.shape[2], res.shape[3] // 2
    kv_cols = kv_all.shape[1]
    cache = (n_tok, kv_cols // 2 // HEAD_DIM, HEAD_DIM)
    hbm = pl.BlockSpec(memory_space=pl.ANY)
    dma = pltpu.SemaphoreType.DMA
    return pl.pallas_call(
        functools.partial(place_kernel, n_tp, n_fsdp),
        out_shape=[jax.ShapeDtypeStruct((n_tok, width), BF16)] + [jax.ShapeDtypeStruct(cache, BF16)] * 2,
        in_specs=[hbm] * 2,
        out_specs=[hbm] * 3,
        scratch_shapes=[pltpu.VMEM((N_ROWCH, N_DOWN, N_REL, sub, c_cols), BF16), pltpu.VMEM((n_tok, width), BF16),
                        pltpu.VMEM((n_tok, kv_cols), BF16), pltpu.VMEM((2, *cache), BF16),
                        dma((N_ROWCH,)), dma((N_ROWCH, N_REL)), dma, dma((2,))],
        compiler_params=pltpu.CompilerParams(vmem_limit_bytes=VMEM_PLACE),
        name="place",
    )(res, kv_all)


def solution(mesh):
    batch_axes = ('dp', 'fsdp')
    n_tp = mesh.shape['tp']
    n_fsdp = mesh.shape['fsdp']
    in_specs = (P(batch_axes, None, None), P(batch_axes, None), P(batch_axes),
                P('fsdp', 'tp'), P('fsdp', 'tp'), P('fsdp', 'tp'), P('tp', 'fsdp'),
                P('fsdp', 'tp'), P('fsdp', 'tp'), P('tp', 'fsdp'), P(None), P(None))
    out_specs = (P(batch_axes, None, None), P(batch_axes, None, 'tp', None), P(batch_axes, None, 'tp', None))

    def local_layer(tokens, positions, valid_len, w_query, w_key, w_value, w_out, w_gate, w_up, w_down, norm_attn, norm_mlp):
        n_tok, width = tokens.shape[1], tokens.shape[2]
        ffn = w_gate.shape[1]
        rows, sub = n_tok // N_ROWCH, n_tok // N_ROWCH // N_REL
        q_cols, kv_cols = w_query.shape[1], w_key.shape[1]
        c_cols = width // N_DOWN
        n_units = 2 * N_DOWN
        freqs = jnp.tile(rope_freqs(), 2)[None]
        vm = pl.BlockSpec(memory_space=pltpu.VMEM)
        smem = pl.BlockSpec(memory_space=pltpu.SMEM)
        hbm = pl.BlockSpec(memory_space=pl.ANY)
        n_groups = 4 + len(GU_SPLIT) - 1 + N_DOWN
        n_y = N_ROWCH + n_units
        st = lambda *s: jax.ShapeDtypeStruct(s, BF16)
        dma = pltpu.SemaphoreType.DMA
        outs = pl.pallas_call(
            functools.partial(layer_kernel, n_tp, n_fsdp),
            out_shape=[st(n_tok, 2 * kv_cols), st(n_units, N_REL, sub, 2 * c_cols),
                       st(width, 2 * kv_cols + q_cols), st(w_out.shape[0], width),
                       st(width, ffn), st(width, ffn), st(N_DOWN, ffn, c_cols), st(n_tok, ffn), st(n_y, 3, sub, width)],
            in_specs=[smem] * 2 + [vm] * 3 + [hbm] * 8,
            out_specs=[hbm] * 9,
            scratch_shapes=[
                pltpu.VMEM((n_tok, width), BF16), pltpu.VMEM((2, width, 2 * TILE), BF16),
                pltpu.VMEM((2, rows, width), BF16),
                pltpu.VMEM((rows, width), BF16), pltpu.VMEM((n_tok, 2 * kv_cols + q_cols), BF16),
                pltpu.VMEM((2, rows, q_cols), BF16), pltpu.VMEM((3, sub, width), BF16),
                pltpu.VMEM((2, sub, 2 * c_cols), BF16), pltpu.VMEM((2, 2 * rows, TILE), BF16),
                pltpu.VMEM((n_tok, HEAD_DIM), F32), pltpu.VMEM((n_tok, HEAD_DIM), F32), pltpu.VMEM((1, n_tok), F32),
                pltpu.VMEM((2, width), F32),
                dma((n_groups,)), dma((n_groups, 4)), dma((n_y, 3)), dma((n_y, 4)),
                dma((4,)), dma((4,)), dma((5,)), dma((2, 11)), dma((2,)), dma((5,)), dma((n_fsdp,)),
            ],
            compiler_params=pltpu.CompilerParams(vmem_limit_bytes=67043328, collective_id=0, has_side_effects=True),
            name="layer",
        )(positions, valid_len, freqs, norm_attn, norm_mlp, tokens[0],
          w_key, w_value, w_query, w_out, w_gate, w_up, w_down)
        kv_all, res = outs[0], outs[1]
        hidden, key_cache, value_cache = place(res, kv_all, n_tok, width, n_tp, n_fsdp)
        return hidden[None], key_cache[None], value_cache[None]

    return jax.shard_map(local_layer, mesh=mesh, in_specs=in_specs, out_specs=out_specs, check_vma=False)
```

```python
import functools
import math
import jax
import jax.numpy as jnp
from jax import lax
from jax.experimental import pallas as pl
from jax.experimental.pallas import tpu as pltpu
from jax.sharding import PartitionSpec as P

HEAD_DIM = 128
ROPE_THETA = 500000.0
NORM_EPS = 1e-5
SCORE_SCALE = HEAD_DIM ** -0.5
LOG2E = 1.4426950408889634
BF16 = jnp.bfloat16
F32 = jnp.float32
N_REL = 4
HALVES = (0, 1)
N_ROWCH = 4
N_DOWN = 4
TILE = 256
GU_SPLIT = (0, 2, 6, 10, 14)
MESH = pl.DeviceIdType.MESH
VMEM_PLACE = 67043328


def rope_freqs():
    half_idx = jnp.arange(HEAD_DIM // 2, dtype=F32)
    inv_freq = jnp.power(ROPE_THETA, -2.0 * half_idx / HEAD_DIM)
    wave_len = 2.0 * math.pi / inv_freq
    smooth = (8192.0 / wave_len - 1.0) / 3.0
    blended = (1.0 - smooth) * inv_freq / 8.0 + smooth * inv_freq
    return jnp.where(wave_len < 2048.0, inv_freq, jnp.where(wave_len > 8192.0, inv_freq / 8.0, blended))


def upto(n):
    return pl.ds(0, n)


def layer_kernel(n_tp, n_fsdp, *refs):
    (pos_ref, len_ref, freq_ref, gain_a, gain_m, tok, wk, wv, wq, wo, wg, wu, wd,
     kv_out, res, full_p, full_o, full_g, full_u, full_d, act, rs,
     u_buf, w_buf, p_buf, x1_buf, qkv_buf, o_buf, stage, r_buf, a_stage, cos_ref, sin_ref, bias_ref, gains,
     x_send, x_recv, y_send, y_recv, w_sem, wd_sem, l_sem, b_sem, a_sem, r_sem, o_sem) = refs
    n_tok, width = tok.shape
    rows = n_tok // N_ROWCH
    sub = rows // N_REL
    k_rows = wk.shape[0]
    kv_cols = wk.shape[1]
    q_cols = wq.shape[1]
    ffn = wg.shape[1]
    o_cols = wo.shape[1]
    d_cols = wd.shape[1] // N_DOWN
    c_cols = d_cols * n_fsdp
    n_x = n_fsdp // 2

    me_t = lax.axis_index("tp")
    me_f = lax.axis_index("fsdp")
    chip, core = me_f // 2, me_f % 2
    t_right = lax.rem(me_t + 1, n_tp)
    t_left = lax.rem(me_t + n_tp - 1, n_tp)
    f_right = 2 * lax.rem(chip + 1, n_x) + core
    f_left = 2 * lax.rem(chip + n_x - 1, n_x) + core
    f_far = 2 * lax.rem(chip + 2, n_x) + core
    other = 1 - 2 * core
    f_twin = me_f + other

    barrier = pltpu.get_barrier_semaphore()
    for peer in ({"tp": t_left}, {"tp": t_right}, {"fsdp": f_left}, {"fsdp": f_right}, {"fsdp": f_twin}):
        pl.semaphore_signal(barrier, inc=1, device_id=peer, device_id_type=MESH)
    pl.semaphore_wait(barrier, 5)

    def al(val, mult):
        return pl.multiple_of(val, mult)

    groups = []

    def add_group(pieces, area):
        groups.append((pieces, area))
        return len(groups) - 1

    def by_rows(full, c0, n):
        return lambda f: full.at[pl.ds(al(f * k_rows, k_rows), k_rows), pl.ds(c0, n)]

    def halves(own, place):
        n = own.shape[0] // 2
        return [(own.at[pl.ds(i * n, n), :], lambda f, i=i: place(f).at[pl.ds(i * n, n), :], i) for i in HALVES]

    def o_piece(f):
        return full_o.at[:, pl.ds(al(f * o_cols, o_cols), o_cols)]

    def d_piece(k, f):
        return full_d.at[k, :, pl.ds(al(f * d_cols, d_cols), d_cols)]

    half_q = q_cols // 2
    q_from = 2 * kv_cols

    def row_area(full, c0, cols):
        return lambda n: full.at[upto(n * k_rows), pl.ds(c0, cols)]

    pkv = add_group([(own, by_rows(full_p, i * kv_cols, kv_cols), i) for i, own in enumerate((wk, wv))], row_area(full_p, 0, q_from))
    q0, q1 = [add_group([(wq.at[:, pl.ds(i * half_q, half_q)], by_rows(full_p, q_from + i * half_q, half_q), i)],
                        row_area(full_p, q_from + i * half_q, half_q)) for i in HALVES]
    po = add_group(halves(wo, o_piece), lambda n: full_o.at[:, upto(n * o_cols)])
    g0, g1, g2, g3 = [
        add_group([(own.at[:, pl.ds(lo * TILE, (hi - lo) * TILE)], by_rows(full, lo * TILE, (hi - lo) * TILE), i)
                   for i, (own, full) in enumerate(((wg, full_g), (wu, full_u)))], row_area(full_g, 0, 2 * (hi - lo) * TILE))
        for lo, hi in zip(GU_SPLIT, GU_SPLIT[1:])]
    d0, d1, d2, d3 = [
        add_group(halves(wd.at[:, pl.ds(k * d_cols, d_cols)], functools.partial(d_piece, k)), lambda n, k=k: full_d.at[k, :, upto(n * d_cols)])
        for k in range(N_DOWN)]

    FIRST, FAR_ON, TWIN = HALVES, 2, 3

    def x_copy(g, i, m):
        own, place, way = groups[g][0][i]
        near = (f_left, f_right)
        if m in FIRST:
            src, owner, target = own, me_f, near[1 - m]
        elif m == FAR_ON:
            owner, target = near[way], near[1 - way]
            src = place(owner)
        else:
            owner, target = (me_f, f_left, f_right, f_far)[m - TWIN], f_twin
            src = own if m == TWIN else place(owner)
        return pltpu.make_async_remote_copy(src_ref=src, dst_ref=place(owner), send_sem=x_send.at[g], recv_sem=x_recv.at[g, min(m, TWIN)],
                                            device_id={"fsdp": target}, device_id_type=MESH)

    def x_all(g, *ms):
        for m in ms:
            for i in range(len(groups[g][0])):
                x_copy(g, i, m).start()

    def x_taken(g, kind, n=1):
        area = groups[g][1](n)
        return pltpu.make_async_remote_copy(src_ref=area, dst_ref=area, send_sem=x_send.at[g], recv_sem=x_recv.at[g, kind],
                                            device_id={"fsdp": f_twin}, device_id_type=MESH)

    def x_first(*gs):
        for g in gs:
            x_all(g, *FIRST, TWIN)

    def x_fwd(g):
        for i, piece in enumerate(groups[g][0]):
            x_taken(g, piece[2]).wait_recv()
            x_copy(g, i, FAR_ON).start()

    def x_side(g):
        if len(groups[g][0]) == 1:
            x_taken(g, 1 - groups[g][0][0][2]).wait_recv()
        x_all(g, TWIN + 1, TWIN + 2)

    def x_second(g):
        x_fwd(g)
        x_side(g)

    def x_third(g):
        x_taken(g, FAR_ON).wait_recv()
        x_all(g, TWIN + 3)

    def x_ready(g):
        x_taken(g, TWIN, 4).wait_recv()

    def x_sent(*gs):
        for g in gs:
            x_taken(g, TWIN, 7).wait_send()

    unit_list = [(k, pair) for pair in range(2) for k in range(N_DOWN)]
    unit_at = [2 * k + pair for k, pair in unit_list]
    unit_order = {u: i for i, u in enumerate(unit_at)}

    def y_rows(e):
        if e < N_ROWCH:
            slot, lane, wid = e % 2, 0, width
        else:
            q = unit_order[e - N_ROWCH] % 4
            slot, lane, wid = q // 2, (q % 2) * (width // 2), 2 * c_cols
        return slot, lane, wid

    def lanes(e, h):
        slot, lane, wid = y_rows(e)
        return slot, pl.ds(lane + h * (wid // 2), wid // 2), pl.ds(h * (wid // 2), wid // 2)

    def g_slice(e, r):
        if e < N_ROWCH:
            return u_buf.at[pl.ds(e * rows + r * sub, sub), :]
        return res.at[e - N_ROWCH, r]

    FAR, NEAR, SUM, RIGHT, LEFT, PASS = range(6)
    OUT, SPREAD, ON = range(3)
    sent_as = (OUT, OUT, OUT, SPREAD, SPREAD, ON)
    GOT_FAR, GOT_SUMS, GOT_SPREAD, GOT_REST = range(4)

    def got_as(e, m, h):
        if m in (RIGHT, LEFT):
            return GOT_SPREAD if e < N_ROWCH or m == LEFT - h else GOT_REST
        return {FAR: GOT_FAR, PASS: GOT_REST}.get(m, GOT_SUMS)

    def y_taken(e, kind, n):
        area = rs.at[e, upto(n), :, upto(y_rows(e)[2])]
        return pltpu.make_async_remote_copy(src_ref=area, dst_ref=area, send_sem=y_send.at[e, min(kind, ON)], recv_sem=y_recv.at[e, kind],
                                            device_id={"tp": t_right}, device_id_type=MESH)

    def y_copy(e, m, h=0):
        slot, here, there = lanes(e, h)
        if m in (RIGHT, LEFT):
            src, dst, to = g_slice(e, 0), g_slice(e, m - 2), m - 3
            if e >= N_ROWCH:
                src, dst = r_buf.at[unit_order[e - N_ROWCH] % 2, :, there], dst.at[:, there]
        elif m == PASS:
            src, dst, to = g_slice(e, 2 - h).at[:, there], g_slice(e, 3).at[:, there], 1 - h
        else:
            r, i, to = {FAR: (3, 0, h), NEAR: (1 + h, 2 - h, 1 - h), SUM: (2 - h, 1 + h, h)}[m]
            src, dst = p_buf.at[slot, pl.ds(r * sub, sub), here], rs.at[e, i, :, there]
        return pltpu.make_async_remote_copy(src_ref=src, dst_ref=dst, send_sem=y_send.at[e, sent_as[m]], recv_sem=y_recv.at[e, got_as(e, m, h)],
                                            device_id={"tp": t_right if to == 0 else t_left}, device_id_type=MESH)

    def rs_slice(e, i):
        return rs.at[e, i, :, upto(y_rows(e)[2])]

    def load_stage(e, idx):
        wid = y_rows(e)[2]
        for i in idx:
            pltpu.make_async_copy(rs_slice(e, i), stage.at[i, :, upto(wid)], l_sem.at[i]).start()

    def wait_stage(e, idx):
        wid = y_rows(e)[2]
        for i in idx:
            pltpu.make_async_copy(rs_slice(e, i), stage.at[i, :, upto(wid)], l_sem.at[i]).wait()

    def y_start(e, hs=HALVES):
        for m in (FAR, NEAR):
            for h in hs:
                y_copy(e, m, h).start()

    def y_have(e):
        y_taken(e, GOT_SUMS, 2).wait_recv()

    def y_send_all(e):
        y_copy(e, LEFT).start()
        y_copy(e, RIGHT).start()

    def y_sent_all(e):
        y_taken(e, SPREAD, 2).wait_send()

    EW = 32

    def y_add(e):
        y_taken(e, GOT_FAR, 1).wait_recv()
        for h in HALVES:
            there = lanes(e, h)[2]
            pltpu.make_async_copy(rs.at[e, 0, :, there], stage.at[0, :, there], l_sem.at[h]).start()
        for h in HALVES:
            slot, here, there = lanes(e, h)
            pltpu.make_async_copy(rs.at[e, 0, :, there], stage.at[0, :, there], l_sem.at[h]).wait()

            def body(i, carry, h=h, here=here, there=there):
                rr = pl.ds(al((2 - h) * sub + i * EW, EW), EW)
                tot = p_buf[slot, rr, here].astype(F32) + stage[0, pl.ds(al(i * EW, EW), EW), there].astype(F32)
                p_buf[slot, rr, here] = tot.astype(BF16)
                return carry

            lax.fori_loop(0, sub // EW, body, 0)
            y_copy(e, SUM, h).start()

    def tok_copy(c):
        row0 = al(c * rows + me_t * sub, sub)
        return pltpu.make_async_copy(tok.at[pl.ds(row0, sub), :], stage.at[0], l_sem.at[3])

    def y_norm(c):
        slot = c % 2
        tok_copy(c).start()
        y_have(c)
        load_stage(c, (1, 2))
        wait_stage(c, (1, 2))
        tok_copy(c).wait()

        def body(i, carry):
            rr = al(i * EW, EW)
            here = pl.ds(rr, EW)
            tot = p_buf[slot, here, :].astype(F32) + stage[1, here, :].astype(F32) + stage[2, here, :].astype(F32)
            x1 = (stage[0, here, :].astype(F32) + tot).astype(BF16)
            x1_buf[pl.ds(al(c * sub + i * EW, EW), EW), :] = x1
            xf = x1.astype(F32)
            inv = lax.rsqrt(jnp.mean(xf * xf, axis=-1, keepdims=True) + NORM_EPS)
            u_buf[pl.ds(al(c * rows + i * EW, EW), EW), :] = (xf * inv * gains[1:, :]).astype(BF16)
            return carry

        lax.fori_loop(0, sub // EW, body, 0)
        y_send_all(c)

    def y_final(k, pair):
        unit = 2 * k + pair
        e = N_ROWCH + unit
        r_slot = unit_order[unit] % 2
        if unit_order[unit] >= 2:
            before = N_ROWCH + unit_at[unit_order[unit] - 2]
            y_sent_all(before)
            r_out(before).wait()
        y_have(e)
        loads = [[pltpu.make_async_copy(rs.at[e, i, :, lanes(e, h)[2]], stage.at[i, :, lanes(e, h)[2]], l_sem.at[2 * h + i - 1])
                  for i in (1, 2)] for h in HALVES]
        for cp in loads[0] + loads[1]:
            cp.start()
        for h in HALVES:
            slot, mine, there = lanes(e, h)
            for cp in loads[h]:
                cp.wait()

            def body(i, carry, h=h, slot=slot, mine=mine):
                here = pl.ds(al(i * EW, EW), EW)
                x_rows = pl.ds(al((2 * pair + h) * sub + i * EW, EW), EW)
                for f in range(n_fsdp):
                    at = pl.ds(h * c_cols + f * d_cols, d_cols)
                    tot = (p_buf[slot, here, pl.ds(mine.start + f * d_cols, d_cols)].astype(F32)
                           + stage[1, here, at].astype(F32) + stage[2, here, at].astype(F32))
                    x1 = x1_buf[x_rows, pl.ds((f * N_DOWN + k) * d_cols, d_cols)].astype(F32)
                    r_buf[r_slot, here, at] = (x1 + tot).astype(BF16)
                return carry

            lax.fori_loop(0, sub // EW, body, 0)
        for m, h in ((LEFT, 0), (RIGHT, 1), (LEFT, 1), (RIGHT, 0)):
            y_copy(e, m, h).start()
        r_out(e).start()

    def r_out(e):
        return pltpu.make_async_copy(r_buf.at[unit_order[e - N_ROWCH] % 2], res.at[e - N_ROWCH, 0], r_sem.at[unit_order[e - N_ROWCH] % 2])

    def y_pass(e):
        y_taken(e, GOT_SPREAD, 2 if e < N_ROWCH else 1).wait_recv()
        for h in HALVES:
            y_copy(e, PASS, h).start()

    def y_ready(e):
        y_taken(e, GOT_REST, 1 if e < N_ROWCH else 2).wait_recv()

    def bounce(src, via, dst, i):
        return pltpu.make_async_copy(src, via, b_sem.at[i]), pltpu.make_async_copy(via, dst, b_sem.at[i])

    small = [
        bounce(wk, w_buf.at[0, upto(k_rows), upto(kv_cols)], by_rows(full_p, 0, kv_cols)(me_f), 0),
        bounce(wv, w_buf.at[0, upto(k_rows), pl.ds(kv_cols, kv_cols)], by_rows(full_p, kv_cols, kv_cols)(me_f), 1),
        bounce(wq.at[:, upto(half_q)], w_buf.at[0, pl.ds(k_rows, k_rows), :], by_rows(full_p, q_from, half_q)(me_f), 2),
        bounce(wq.at[:, pl.ds(half_q, half_q)], w_buf.at[0, pl.ds(2 * k_rows, k_rows), :], by_rows(full_p, q_from + half_q, half_q)(me_f), 3),
        bounce(wo, w_buf.at[0, pl.ds(3 * k_rows, wo.shape[0]), :], o_piece(me_f), 4),
    ] + [
        bounce(wd.at[:, pl.ds(k * d_cols, d_cols)], w_buf.at[1, upto(ffn), pl.ds(k * d_cols, d_cols)], d_piece(k, me_f), 5 + k)
        for k in range(N_DOWN)
    ]
    large = [
        bounce(wg, p_buf.at[0, :, upto(ffn)], by_rows(full_g, 0, ffn)(me_f), 9),
        bounce(wu, p_buf.at[1, :, upto(ffn)], by_rows(full_u, 0, ffn)(me_f), 10),
    ]

    def bounce_in(group):
        for a, _ in group:
            a.start()

    def bounce_out(group):
        for a, b in group:
            a.wait()
            b.start()

    def bounce_end(group):
        for _, b in group:
            b.wait()

    def norm_rows(late):
        n_tile = n_tok // rows

        def load(i):
            return pltpu.make_async_copy(tok.at[pl.ds(i * rows, rows), :], p_buf.at[i % 2], w_sem.at[i % 2])

        load(0).start()
        for i in range(n_tile):
            if i + 1 < n_tile:
                load(i + 1).start()
            load(i).wait()

            def body(j, carry, i=i):
                vals = p_buf[i % 2, pl.ds(al(j * EW, EW), EW), :].astype(F32)
                inv = lax.rsqrt(jnp.mean(vals * vals, axis=-1, keepdims=True) + NORM_EPS)
                u_buf[pl.ds(al(i * rows + j * EW, EW), EW), :] = (vals * inv * gains[:1, :]).astype(BF16)
                return carry

            lax.fori_loop(0, rows // EW, body, 0)
            if i == n_tile - 2:
                late()

    def tables():
        sign = jnp.where(lax.broadcasted_iota(jnp.int32, (1, HEAD_DIM), 1) < HEAD_DIM // 2, -1.0, 1.0)
        first = pos_ref[0, 0]

        def body(i, carry):
            here = pl.ds(al(i * sub, sub), sub)
            row = first + i * sub + lax.broadcasted_iota(jnp.int32, (sub, HEAD_DIM), 0)
            angle = row.astype(F32) * freq_ref[...]
            cos_ref[here, :] = jnp.cos(angle)
            sin_ref[here, :] = sign * jnp.sin(angle)
            return carry

        lax.fori_loop(0, n_tok // sub, body, 0)
        key = lax.broadcasted_iota(jnp.int32, (1, n_tok), 1)
        bias_ref[...] = jnp.where(key < len_ref[0], 0.0, -jnp.inf)

    def stream(n0, n1, load, compute, hooks={}, lazy=(), fetched=False, then=None):
        def fetch(n, slot):
            for cp in load(n, slot):
                cp.start()

        if not fetched:
            fetch(n0, 0)

        def body(n, carry):
            slot = lax.rem(n - n0, 2)
            late = functools.reduce(jnp.logical_or, [n + 1 == at for at in lazy], n + 1 >= n1)
            pl.when(jnp.logical_not(late))(lambda: fetch(n + 1, 1 - slot))
            if then:
                pl.when(n + 1 == n1)(then)
            for cp in load(n, slot):
                cp.wait()
            compute(n, slot)
            for at, todo in hooks.items():
                @pl.when(n == at)
                def _(at=at, todo=todo):
                    todo()
                    if at + 1 in lazy:
                        fetch(at + 1, 1 - slot)
            return carry

        lax.fori_loop(n0, n1, body, 0)

    def project(hooks, lazy):
        def load(n, slot):
            return (pltpu.make_async_copy(full_p.at[:, pl.ds(al(n * TILE, TILE), TILE)], w_buf.at[slot, :, upto(TILE)], w_sem.at[slot]),)

        def compute(n, slot):
            plain = n == 1

            def body(m, carry):
                here = pl.ds(al(m * 2 * rows, rows), 2 * rows)
                acc = jnp.dot(u_buf[here, :], w_buf[slot, :, :TILE], preferred_element_type=F32)
                cos_t = jnp.where(plain, 1.0, cos_ref[here, :])
                sin_t = jnp.where(plain, 0.0, sin_ref[here, :])
                for h in range(TILE // HEAD_DIM):
                    val = acc[:, h * HEAD_DIM:(h + 1) * HEAD_DIM]
                    val = val * cos_t + pltpu.roll(val, HEAD_DIM // 2, 1) * sin_t
                    qkv_buf[here, pl.ds(al(n * TILE + h * HEAD_DIM, HEAD_DIM), HEAD_DIM)] = val.astype(BF16)
                return carry

            lax.fori_loop(0, n_tok // (2 * rows), body, 0)

        stream(0, full_p.shape[1] // TILE, load, compute, hooks, lazy)

    def attend(c, mid=None):
        blk = 2 * sub
        n_blk = rows // blk
        n_old = c * rows
        n_head = q_cols // HEAD_DIM
        per_grp = q_cols // kv_cols
        dims = (((1,), (1,)), ((), ()))
        here = pl.ds(n_old, rows)

        def body(idx, carry):
            head = idx // n_blk
            part = lax.rem(idx, n_blk)
            row0 = al(part * blk, blk)
            col0 = al(head * HEAD_DIM, HEAD_DIM)
            k_at = al((head // per_grp) * HEAD_DIM, HEAD_DIM)
            k_cols, v_cols = pl.ds(k_at, HEAD_DIM), pl.ds(al(kv_cols + k_at, HEAD_DIM), HEAD_DIM)
            q_blk = qkv_buf[pl.ds(al(n_old + row0, blk), blk), pl.ds(al(q_from + col0, HEAD_DIM), HEAD_DIM)]
            s_new = lax.dot_general(q_blk, qkv_buf[here, k_cols], dims, preferred_element_type=F32)
            s_new = s_new * (SCORE_SCALE * LOG2E) + bias_ref[:, here]
            q_idx = row0 + lax.broadcasted_iota(jnp.int32, (blk, rows), 0)
            k_idx = lax.broadcasted_iota(jnp.int32, (blk, rows), 1)
            s_new = jnp.where(k_idx <= q_idx, s_new, -jnp.inf)
            top = jnp.max(s_new, axis=1, keepdims=True)
            if n_old:
                s_old = lax.dot_general(q_blk, qkv_buf[:n_old, k_cols], dims, preferred_element_type=F32)
                s_old = s_old * (SCORE_SCALE * LOG2E) + bias_ref[:, :n_old]
                top = jnp.maximum(top, jnp.max(s_old, axis=1, keepdims=True))
            p_new = jnp.exp2(s_new - top)
            den = jnp.sum(p_new, axis=1, keepdims=True)
            acc = jnp.dot(p_new.astype(BF16), qkv_buf[here, v_cols], preferred_element_type=F32)
            if n_old:
                p_old = jnp.exp2(s_old - top)
                den = den + jnp.sum(p_old, axis=1, keepdims=True)
                acc = acc + jnp.dot(p_old.astype(BF16), qkv_buf[:n_old, v_cols], preferred_element_type=F32)
            out = (acc / den).astype(BF16)
            for s in range(blk // sub):
                dist = lax.rem(part * (blk // sub) + s - me_t + n_tp, n_tp)
                pos = jnp.where(dist == 0, 0, jnp.where(dist == n_tp - 1, 1, dist + 1))
                o_buf[c % 2, pl.ds(al(pos * sub, sub), sub), pl.ds(col0, HEAD_DIM)] = out[s * sub:(s + 1) * sub, :]
            if mid:
                pl.when(idx == n_head)(mid)
            return carry

        lax.fori_loop(0, n_head * n_blk, body, 0)

    def o_place(n):
        depth = wo.shape[0]
        per = width // depth
        return n // per, pl.ds(al(lax.rem(n, per) * depth, depth), depth)

    def o_tile(n):
        slot, here = o_place(n)
        return pltpu.make_async_copy(full_o.at[:, pl.ds(al(n * o_cols, o_cols), o_cols)], w_buf.at[slot, here, :], o_sem.at[n])

    def out_load():
        def body(n, carry):
            o_tile(n).start()
            return carry

        lax.fori_loop(0, n_fsdp, body, 0)

    def out_project(c):
        def body(n, carry):
            if c == 0:
                o_tile(n).wait()
            slot, here = o_place(n)
            acc = jnp.dot(o_buf[c % 2], w_buf[slot, here, :], preferred_element_type=F32)
            p_buf[c % 2, :, pl.ds(al(n * o_cols, o_cols), o_cols)] = acc.astype(BF16)
            return carry

        lax.fori_loop(0, n_fsdp, body, 0)

    def act_copy(c0, nc, n, slot):
        return pltpu.make_async_copy(a_stage.at[slot, upto(nc * rows), :],
                                     act.at[pl.ds(c0 * rows, nc * rows), pl.ds(al(n * TILE, TILE), TILE)], a_sem.at[slot])

    def gate_up(pair, n0, n1, hooks={}):
        c0, nc = 2 * pair, 2
        def load(n, slot):
            here = pl.ds(al(n * TILE, TILE), TILE)
            return (pltpu.make_async_copy(full_g.at[:, here], w_buf.at[slot, :, upto(TILE)], w_sem.at[slot]),
                    pltpu.make_async_copy(full_u.at[:, here], w_buf.at[slot, :, pl.ds(TILE, TILE)], w_sem.at[2 + slot]))

        def compute(n, slot):
            lhs = u_buf[c0 * rows:(c0 + nc) * rows, :]
            gate = jnp.dot(lhs, w_buf[slot, :, :TILE], preferred_element_type=F32)
            gate = gate * jax.nn.sigmoid(gate)
            val = gate * jnp.dot(lhs, w_buf[slot, :, TILE:], preferred_element_type=F32)

            @pl.when(n - n0 >= 2)
            def _():
                act_copy(c0, nc, n, slot).wait()
            a_stage[slot, :nc * rows, :] = val.astype(BF16)
            act_copy(c0, nc, n, slot).start()

        stream(n0, n1, load, compute, hooks)
        for i in range(min(2, n1 - n0)):
            act_copy(c0, nc, n1 - 1, (n1 - 1 - i - n0) % 2).wait()

    def load_act(c):
        here = pl.ds(c * rows, rows)
        return pltpu.make_async_copy(act.at[here, :], u_buf.at[here, upto(ffn)], r_sem.at[3 + c % 2])

    def down_place(slot, i):
        return upto(ffn // 2), pl.ds(al((2 * slot + i) * TILE, TILE), TILE)

    def down_tile(k, n, slot):
        return [pltpu.make_async_copy(full_d.at[k, pl.ds(i * (ffn // 2), ffn // 2), pl.ds(al(n * TILE, TILE), TILE)],
                                      qkv_buf.at[down_place(slot, i)], wd_sem.at[2 * slot + i]) for i in HALVES]

    def down_fetch(k):
        for cp in down_tile(k, 0, 0):
            cp.start()

    def down(k, pair, cs, fetched, then):
        e = N_ROWCH + 2 * k + pair
        slot_p, lane, _ = y_rows(e)
        half = ffn // 2
        row0, n_row = (2 * pair + cs[0]) * rows, len(cs) * rows

        def compute(n, slot):
            prod = sum(jnp.dot(u_buf[row0:row0 + n_row, i * half:(i + 1) * half], qkv_buf[down_place(slot, i)], preferred_element_type=F32)
                       for i in HALVES).astype(BF16)
            for i, ci in enumerate(cs):
                p_buf[slot_p, :, pl.ds(al(lane + ci * c_cols + n * TILE, TILE), TILE)] = prod[i * rows:(i + 1) * rows, :]

        stream(0, c_cols // TILE, functools.partial(down_tile, k), compute, fetched=fetched, then=then)

    def sent(e):
        y_taken(e, OUT, 3).wait_send()

    def passed(e):
        y_taken(e, ON, 1).wait_send()

    def scoped(fn):
        def run(*args, **kw):
            with jax.named_scope("_".join([fn.__name__] + [str(a) for a in args if isinstance(a, int)])):
                return fn(*args, **kw)
        return run

    x_first, x_fwd, x_side, x_third, x_ready = map(scoped, (x_first, x_fwd, x_side, x_third, x_ready))
    y_start, y_add, y_norm, y_final, y_pass, y_ready = map(scoped, (y_start, y_add, y_norm, y_final, y_pass, y_ready))
    norm_rows, project, attend, out_project, gate_up, down = map(scoped, (norm_rows, project, attend, out_project, gate_up, down))
    tables, bounce_in, bounce_out, bounce_end, sent = map(scoped, (tables, bounce_in, bounce_out, bounce_end, sent))

    def x_done(g):
        x_third(g)
        x_ready(g)

    def sent_u(*cs):
        for c in cs:
            y_sent_all(c)
            passed(c)

    c0, c1, c2, c3 = range(N_ROWCH)
    units = [N_ROWCH + u for u in unit_at]
    t0, t1, t2, t3, t4 = GU_SPLIT

    def begin(i, fetched=False, ahead=False, wait=None):
        if i >= 4:
            sent(units[i - 4])
        k, pair = unit_list[i]
        parts = [(h,) for h in HALVES] if wait else (HALVES,)
        for cs in parts:
            last = cs == parts[-1]
            then = functools.partial(down_fetch, unit_list[i + 1][0]) if last and ahead else None if last else functools.partial(down_fetch, k)
            if wait:
                wait(cs[0])
            down(k, pair, cs, fetched or cs != parts[0], then)
            y_start(units[i], cs)

    x_first(pkv, q0)
    bounce_in(small)
    gains[:1, :] = gain_a[...].astype(F32)[None]
    gains[1:, :] = gain_m[...].astype(F32)[None]
    norm_rows(lambda: x_second(pkv))
    bounce_out(small)
    bounce_in(large)
    tables()
    x_fwd(q0)
    x_first(q1)
    x_done(pkv)
    bounce_end(small)
    kv_copy = pltpu.make_async_copy(qkv_buf.at[:, upto(q_from)], kv_out, r_sem.at[2])

    def have_kv():
        bounce_out(large)
        kv_copy.start()
        x_side(q0)
        x_done(q0)

    project({
        0: lambda: (x_fwd(q1), x_first(po)),
        1: have_kv,
        3: lambda: (x_side(q1), x_done(q1)),
        4: lambda: (x_second(po), x_first(g0, g1, g2)),
    }, (2, 4))
    attend(c0)
    x_done(po)
    out_load()
    bounce_end(large)
    out_project(c0)
    y_start(c0)
    attend(c1)
    out_project(c1)
    y_start(c1)
    x_second(g0)
    attend(c2, lambda: y_add(c0))
    attend(c3, lambda: y_add(c1))
    x_second(g1)
    y_norm(c0)
    y_norm(c1)
    sent(c0)
    out_project(c2)
    sent(c1)
    out_project(c3)
    y_pass(c0)
    y_pass(c1)
    y_start(c2)
    y_start(c3)
    x_second(g2)
    x_first(g3)
    x_third(g0)
    x_third(g1)
    x_ready(g0)
    y_ready(c0)
    y_ready(c1)
    x_ready(g1)
    gate_up(0, t0, t3, {t1: lambda: (x_third(g2), y_add(c2)), t2 - 2: lambda: x_ready(g2), t2 + 1: lambda: y_add(c3)})
    x_second(g3)
    x_first(d0)
    y_norm(c2)
    y_norm(c3)
    x_done(g3)
    y_pass(c2)
    gate_up(0, t3, t4, {t3 + 1: lambda: (x_second(d0), x_first(d1)), t4 - 2: lambda: y_pass(c3)})
    sent_u(c0, c1)
    load_act(c0).start()
    load_act(c1).start()
    kv_copy.wait()
    x_done(d0)
    down_fetch(0)
    sent(c2)
    sent(c3)
    (load_act(c0).wait(), load_act(c1).wait(), begin(0, True))
    x_second(d1)
    x_first(d2)
    y_ready(c2)
    y_ready(c3)
    sent_u(c2, c3)
    f0, f1, f2, f3 = units[:N_DOWN]
    gate_up(1, t0, t4, {
        1: lambda: (y_add(f0), x_done(d1), begin(1), y_final(*unit_list[0])),
        3: lambda: (y_add(f1), x_second(d2), x_first(d3)),
        5: lambda: x_third(d2),
        6: lambda: (y_pass(f0), y_final(*unit_list[1]), x_ready(d2), begin(2), x_second(d3)),
        8: lambda: y_pass(f1),
        9: lambda: (y_add(f2), x_done(d3), begin(3)),
        10: lambda: y_final(*unit_list[2]),
        12: lambda: (y_add(f3), down_fetch(0)),
    })
    load_act(c2).start()
    load_act(c3).start()
    y_pass(f2)
    n_unit = len(units)
    half = n_unit // 2
    begin(half, True, True, lambda h: load_act(2 + h).wait())
    y_final(*unit_list[half - 1])
    for i in range(half, n_unit):
        if i + 1 < n_unit:
            begin(i + 1, True, i + 2 < n_unit)
        if i == half:
            y_add(units[i])
        x_sent(*range(len(groups) * (i - half) // half, len(groups) * (i + 1 - half) // half))
        y_pass(units[i - 1])
        if i > half:
            y_ready(units[i - 2])
            passed(units[i - 2])
        if i + 1 < n_unit:
            y_add(units[i + 1])
        y_final(*unit_list[i])
    for e in units[-4:]:
        sent(e)
    y_pass(units[-1])
    for e in units[:half - 1] + units[-2:]:
        y_ready(e)
        passed(e)
    for e in units[-2:]:
        y_sent_all(e)
        r_out(e).wait()


def place_kernel(n_tp, n_fsdp, res, kv, out, key_out, value_out, in_buf, out_buf, kv_buf, cache_buf, in_sem, out_sem, kv_sem, cache_sem):
    sub, c_cols = res.shape[2], res.shape[3] // 2
    cols = c_cols // n_fsdp
    me_t = lax.axis_index("tp")

    def load(c, k):
        src = res.at[2 * k + c // 2, :, :, pl.ds(pl.multiple_of(lax.rem(c, 2) * c_cols, c_cols), c_cols)]
        return pltpu.make_async_copy(src, in_buf.at[c, k], in_sem.at[c])

    def store(c, r):
        here = pl.ds(pl.multiple_of((c * N_REL + r) * sub, sub), sub)
        return pltpu.make_async_copy(out_buf.at[here, :], out.at[here, :], out_sem.at[c, r])

    def caches():
        return [pltpu.make_async_copy(cache_buf.at[i], dst, cache_sem.at[i]) for i, dst in enumerate((key_out, value_out))]

    for c in range(N_ROWCH):
        for k in range(N_DOWN):
            load(c, k).start()
    kv_load = pltpu.make_async_copy(kv, kv_buf, kv_sem)
    kv_load.start()

    def chunk(c, carry):
        pltpu.make_async_copy(res.at[upto(N_DOWN), :, :, upto(c_cols)], in_buf.at[c], in_sem.at[c]).wait()
        for r, dist in enumerate((0, n_tp - 1, 1, 2)):
            row = lax.rem(me_t + dist, n_tp)
            here = pl.ds(pl.multiple_of((c * N_REL + row) * sub, sub), sub)
            for k in range(N_DOWN):
                for f in range(n_fsdp):
                    c0 = (f * N_DOWN + k) * cols
                    out_buf[here, c0:c0 + cols] = in_buf[c, k, r, :, f * cols:(f + 1) * cols]
            store(c, row).start()
        return carry

    lax.fori_loop(0, N_ROWCH, chunk, 0)
    kv_load.wait()
    for i in HALVES:
        n = kv.shape[1] // 2
        cache_buf[i] = kv_buf[:, i * n:(i + 1) * n].reshape(cache_buf.shape[1:])
    for cp in caches():
        cp.start()

    def finish(c, carry):
        for r in range(N_REL):
            store(c, r).wait()
        return carry

    lax.fori_loop(0, N_ROWCH, finish, 0)
    for cp in caches():
        cp.wait()


def place(res, kv_all, n_tok, width, n_tp, n_fsdp):
    sub, c_cols = res.shape[2], res.shape[3] // 2
    kv_cols = kv_all.shape[1]
    cache = (n_tok, kv_cols // 2 // HEAD_DIM, HEAD_DIM)
    hbm = pl.BlockSpec(memory_space=pl.ANY)
    dma = pltpu.SemaphoreType.DMA
    return pl.pallas_call(
        functools.partial(place_kernel, n_tp, n_fsdp),
        out_shape=[jax.ShapeDtypeStruct((n_tok, width), BF16)] + [jax.ShapeDtypeStruct(cache, BF16)] * 2,
        in_specs=[hbm] * 2,
        out_specs=[hbm] * 3,
        scratch_shapes=[pltpu.VMEM((N_ROWCH, N_DOWN, N_REL, sub, c_cols), BF16), pltpu.VMEM((n_tok, width), BF16),
                        pltpu.VMEM((n_tok, kv_cols), BF16), pltpu.VMEM((2, *cache), BF16),
                        dma((N_ROWCH,)), dma((N_ROWCH, N_REL)), dma, dma((2,))],
        compiler_params=pltpu.CompilerParams(vmem_limit_bytes=VMEM_PLACE),
        name="place",
    )(res, kv_all)


def solution(mesh):
    batch_axes = ('dp', 'fsdp')
    n_tp = mesh.shape['tp']
    n_fsdp = mesh.shape['fsdp']
    in_specs = (P(batch_axes, None, None), P(batch_axes, None), P(batch_axes),
                P('fsdp', 'tp'), P('fsdp', 'tp'), P('fsdp', 'tp'), P('tp', 'fsdp'),
                P('fsdp', 'tp'), P('fsdp', 'tp'), P('tp', 'fsdp'), P(None), P(None))
    out_specs = (P(batch_axes, None, None), P(batch_axes, None, 'tp', None), P(batch_axes, None, 'tp', None))

    def local_layer(tokens, positions, valid_len, w_query, w_key, w_value, w_out, w_gate, w_up, w_down, norm_attn, norm_mlp):
        n_tok, width = tokens.shape[1], tokens.shape[2]
        ffn = w_gate.shape[1]
        rows, sub = n_tok // N_ROWCH, n_tok // N_ROWCH // N_REL
        q_cols, kv_cols = w_query.shape[1], w_key.shape[1]
        c_cols = width // N_DOWN
        n_units = 2 * N_DOWN
        freqs = jnp.tile(rope_freqs(), 2)[None]
        vm = pl.BlockSpec(memory_space=pltpu.VMEM)
        smem = pl.BlockSpec(memory_space=pltpu.SMEM)
        hbm = pl.BlockSpec(memory_space=pl.ANY)
        n_groups = 4 + len(GU_SPLIT) - 1 + N_DOWN
        n_y = N_ROWCH + n_units
        st = lambda *s: jax.ShapeDtypeStruct(s, BF16)
        dma = pltpu.SemaphoreType.DMA
        outs = pl.pallas_call(
            functools.partial(layer_kernel, n_tp, n_fsdp),
            out_shape=[st(n_tok, 2 * kv_cols), st(n_units, N_REL, sub, 2 * c_cols),
                       st(width, 2 * kv_cols + q_cols), st(w_out.shape[0], width),
                       st(width, ffn), st(width, ffn), st(N_DOWN, ffn, c_cols), st(n_tok, ffn), st(n_y, 3, sub, width)],
            in_specs=[smem] * 2 + [vm] * 3 + [hbm] * 8,
            out_specs=[hbm] * 9,
            scratch_shapes=[
                pltpu.VMEM((n_tok, width), BF16), pltpu.VMEM((2, width, 2 * TILE), BF16),
                pltpu.VMEM((2, rows, width), BF16),
                pltpu.VMEM((rows, width), BF16), pltpu.VMEM((n_tok, 2 * kv_cols + q_cols), BF16),
                pltpu.VMEM((2, rows, q_cols), BF16), pltpu.VMEM((3, sub, width), BF16),
                pltpu.VMEM((2, sub, 2 * c_cols), BF16), pltpu.VMEM((2, 2 * rows, TILE), BF16),
                pltpu.VMEM((n_tok, HEAD_DIM), F32), pltpu.VMEM((n_tok, HEAD_DIM), F32), pltpu.VMEM((1, n_tok), F32),
                pltpu.VMEM((2, width), F32),
                dma((n_groups,)), dma((n_groups, 4)), dma((n_y, 3)), dma((n_y, 4)),
                dma((4,)), dma((4,)), dma((5,)), dma((11,)), dma((2,)), dma((5,)), dma((n_fsdp,)),
            ],
            compiler_params=pltpu.CompilerParams(vmem_limit_bytes=67043328, collective_id=0, has_side_effects=True),
            name="layer",
        )(positions, valid_len, freqs, norm_attn, norm_mlp, tokens[0],
          w_key, w_value, w_query, w_out, w_gate, w_up, w_down)
        kv_all, res = outs[0], outs[1]
        hidden, key_cache, value_cache = place(res, kv_all, n_tok, width, n_tp, n_fsdp)
        return hidden[None], key_cache[None], value_cache[None]

    return jax.shard_map(local_layer, mesh=mesh, in_specs=in_specs, out_specs=out_specs, check_vma=False)
```
